32 devices in a mesh: groups: 2 (over x), seq: 16 (over z, y, core).
Axes of the slice: x: 2, y: 2, z: 4, core: 2. Of those that a mesh axis runs over, the one named last changes fastest.
Arguments:
- queries: bfloat16 [2048, 24576], P(('groups', 'seq')), parts along dimension 0, may hold values from -500 to 500
- kv_new: bfloat16 [2048, 576], P(('groups', 'seq')), parts along dimension 0, may hold values from -6 to 6
- kv_cache: bfloat16 [1024, 576], P(('groups', 'seq')), parts along dimension 0, may hold values from -6 to 6
- kv_gain: float32 [512], replicated, may hold values from 0.5 to 2
- w_key: bfloat16 [512, 16384], P(None, 'seq'), may hold values from -0.25 to 0.25
- w_value: bfloat16 [512, 16384], P(None, 'seq'), may hold values from -0.25 to 0.25
- prefix_len: int32 [2], P('groups'), parts along dimension 0, may hold values from 128 to 512
Outputs:
- attended: bfloat16 [2048, 16384], P(('groups', 'seq')), parts along dimension 0
The draws below stay inside these ranges and needn't reach their ends.
There are 2 independent parts, one for each index of `groups`. The reference program is written for one: setup_inputs(seed, part) draws one part's arguments, and reference() takes and returns one part's arrays. A program takes and returns all parts, laid end to end along the dimension named above; an argument that names none is the same for every part. Nothing has to cross between parts.
Inputs may be any that keep to these rules, and one draw needn't show every extreme that they name: The stretch's tokens take positions from prefix_len on.
All inputs are finite; a program needn't handle non-finite values.
Results may differ from the reference program's by a relative error of at most 0.012.
Values may be sent and summed in bfloat16 or wider, within the bound.
A program may use at most 128 MiB of HBM per device.

```python
import math
import jax
import jax.numpy as jnp
from jax import lax

H = 128
NOPE = 128
ROPE = 64
LATENT = 512
VH = 128
TOKENS = 1024
CACHE = 512


def draw_queries(key, part):
    base_key = jax.random.fold_in(jax.random.fold_in(key, 11), 0)
    values = jnp.clip(jax.random.normal(base_key, (TOKENS, H * (NOPE + ROPE)), jnp.float32), -8.0, 8.0)
    return values.astype(jnp.bfloat16)


def block_scale(rng, extent, shards, least, top_value):
    def one(position, blocks):
        draws = jax.random.uniform(jax.random.fold_in(jax.random.fold_in(rng, 6), position), (blocks,), jnp.float32, least / len(shards), top_value / len(shards))
        return jnp.repeat(jnp.exp(draws), extent[position] // blocks).reshape((-1,) + (1,) * (len(extent) - position - 1))

    loudness = one(*shards[0])
    for cut in shards[1:]:
        loudness = loudness * one(*cut)
    return loudness


def normal_values(stream_key, extent, deviation, reach, cuts=(), kind=jnp.bfloat16):
    result = deviation * jax.random.normal(stream_key, extent, jnp.float32)
    if cuts:
        result = result * block_scale(stream_key, extent, cuts, -0.22, 0.18)
    return jnp.clip(result, -reach, reach).astype(kind)


def setup_inputs(seed: int = 0, part: int = 0) -> dict:
    arg_keys = jax.random.split(jax.random.key(seed), 8)
    part_splits = jax.random.split(jax.random.fold_in(arg_keys[7], part), 8)
    return {
        "queries": draw_queries(jax.random.fold_in(jax.random.fold_in(arg_keys[7], part), 71), part),
        "kv_new": normal_values(part_splits[1], (TOKENS, LATENT + ROPE), 1.0, 6.0, ((0, 16),)),
        "kv_cache": normal_values(part_splits[2], (CACHE, LATENT + ROPE), 1.0, 6.0, ((0, 16),)),
        "kv_gain": jnp.clip(jnp.exp(jax.random.uniform(arg_keys[3], (LATENT,), jnp.float32, math.log(0.5), math.log(2.0))), 0.5, 2.0),
        "w_key": normal_values(arg_keys[4], (LATENT, H * NOPE), LATENT ** -0.5, 0.25, ((1, 16),)),
        "w_value": normal_values(arg_keys[5], (LATENT, H * VH), LATENT ** -0.5, 0.25, ((1, 16),)),
        "prefix_len": jax.random.randint(part_splits[6], (1,), CACHE // 4, CACHE + 1).astype(jnp.int32),
    }


epsilon = 1e-06

def phases_for(positions, rope_width):
    half_width = rope_width // 2
    inverse = 10000.0 ** (-(jnp.arange(half_width, dtype=jnp.float32) * 2.0) / rope_width)
    return positions.astype(jnp.float32)[:, None] * inverse[None, :]

def rotate(values, phases):
    half_width = values.shape[-1] // 2
    front_half = values[..., :half_width]
    back_half = values[..., half_width:]
    cosine = jnp.cos(phases)
    sine_part = jnp.sin(phases)
    return jnp.concatenate([front_half * cosine - back_half * sine_part, back_half * cosine + front_half * sine_part], -1)

def reference(queries, kv_new, kv_cache, kv_gain, w_key, w_value, prefix_len):
    stretch_start = prefix_len[0]
    tokens_all = queries.shape[0]
    cached_all = kv_cache.shape[0]
    positions = stretch_start + jnp.arange(tokens_all, dtype=jnp.int32)
    phases = phases_for(positions, ROPE)
    raw_latent = kv_new[:, :LATENT].astype(jnp.float32)
    inv_rms = lax.rsqrt(lax.optimization_barrier(jnp.mean(raw_latent * raw_latent, axis=1, keepdims=True)) + epsilon)
    latent_new = (raw_latent * inv_rms * kv_gain[None, :]).astype(jnp.bfloat16)
    rope_new = rotate(kv_new[:, LATENT:].astype(jnp.float32), phases).astype(jnp.bfloat16)
    keys_all = jnp.concatenate([kv_cache, jnp.concatenate([latent_new, rope_new], 1)], 0)
    latent_all = keys_all[:, :LATENT]
    key_rope = keys_all[:, LATENT:]
    query_heads = queries.reshape(tokens_all, H, NOPE + ROPE)
    query_rot = rotate(query_heads[:, :, NOPE:].astype(jnp.float32), phases[:, None, :]).astype(jnp.bfloat16)
    query_nope = jnp.transpose(query_heads[:, :, :NOPE], (1, 0, 2))
    query_rot = jnp.transpose(query_rot, (1, 0, 2))
    key_maps = jnp.transpose(w_key.reshape(LATENT, H, NOPE), (1, 0, 2))
    value_maps = jnp.transpose(w_value.reshape(LATENT, H, VH), (1, 0, 2))
    key_index = jnp.arange(cached_all + tokens_all, dtype=jnp.int32)[None, :]
    row_index = jnp.arange(tokens_all, dtype=jnp.int32)[:, None]
    live_mask = jnp.where(key_index < cached_all, key_index < stretch_start, key_index - cached_all <= row_index)
    score_scale = 1.0 / math.sqrt(NOPE + ROPE)

    def one_head(operands):
        head_nope, head_rot, key_map, value_map = operands
        key_nope = jnp.dot(latent_all, key_map, preferred_element_type=jnp.float32).astype(jnp.bfloat16)
        value_rows = jnp.dot(latent_all, value_map, preferred_element_type=jnp.float32).astype(jnp.bfloat16)
        scores = jnp.dot(head_nope, key_nope.T, preferred_element_type=jnp.float32)
        scores = scores + jnp.dot(head_rot, key_rope.T, preferred_element_type=jnp.float32)
        scores = jnp.where(live_mask, scores * score_scale, -1e+30)
        top_score = lax.optimization_barrier(jnp.max(scores, axis=1, keepdims=True))
        exp_scores = jnp.exp(scores - top_score)
        weights = (exp_scores / lax.optimization_barrier(jnp.sum(exp_scores, axis=1, keepdims=True))).astype(jnp.bfloat16)
        return jnp.dot(weights, value_rows, preferred_element_type=jnp.float32).astype(jnp.bfloat16)
    outputs = lax.map(one_head, (query_nope, query_rot, key_maps, value_maps))
    return jnp.transpose(outputs, (1, 0, 2)).reshape(tokens_all, H * VH)
```

```python
import functools
import math

import jax
import jax.numpy as jnp
from jax import lax
from jax.experimental import pallas as pl
from jax.experimental.pallas import tpu as pltpu
from jax.sharding import PartitionSpec as P

NOPE = 128
ROPE = 64
LATENT = 512
VH = 128
WIDTH = NOPE + ROPE
INNER = 4

epsilon = 1e-06


def exclusive(a, b, extent):
    result = 0
    bit = 1
    while bit < extent:
        result = result + ((a // bit + b // bit) % 2) * bit
        bit *= 2
    return result


def inverse_lanes():
    half = ROPE // 2
    inverse = 10000.0 ** (-(jnp.arange(half, dtype=jnp.float32) * 2.0) / ROPE)
    return jnp.concatenate([inverse] * 4)[None, :]


def swap_halves(x, lane):
    return jnp.where(lane % ROPE < ROPE // 2, pltpu.roll(x, 96, 1), pltpu.roll(x, 32, 1))


def kernel(
    n, tok, cac, heads, chunks,
    q_hbm, kvn_hbm, kvc_hbm, wk_hbm, wv_hbm, gain_ref, inverse_ref, plen_ref,
    out_hbm,
    qbuf, kvn, kvc, weights, keys, vals, bias, obuf, cos_ref, sin_ref,
    local_sem, own_out_sem, q_send, q_recv, kv_send, kv_recv, o_send, o_recv, w_send, w_recv,
):
    me = lax.axis_index("seq")
    part = lax.axis_index("groups")
    piece = part % 2
    half = n // 2
    mirror = (me + half) % n
    half_first = (me // half) * half
    half_slabs = half // INNER
    slab = me // INNER
    inner = me % INNER
    slabs = n // INNER
    T, C = n * tok, n * cac
    S = T + C
    qw = heads * WIDTH
    ow = heads * VH
    rows = INNER * tok
    f32, bf16 = jnp.float32, jnp.bfloat16

    def blk(ref, b, size):
        return ref.at[pl.ds(pl.multiple_of(b * size, size), size), :]

    def cols(ref, b, size):
        return ref.at[:, pl.ds(pl.multiple_of(b * size, 128), size)]

    own = [
        pltpu.make_async_copy(kvn_hbm, blk(kvn, me, tok), local_sem.at[0]),
        pltpu.make_async_copy(kvc_hbm, blk(kvc, me, cac), local_sem.at[1]),
        pltpu.make_async_copy(wk_hbm, weights.at[0, 0], local_sem.at[2]),
        pltpu.make_async_copy(wv_hbm, weights.at[1, 0], local_sem.at[3]),
        pltpu.make_async_copy(
            cols(q_hbm, me, qw), blk(qbuf.at[0], me - half_first, tok), local_sem.at[4]
        ),
        pltpu.make_async_copy(
            cols(q_hbm, mirror, qw), blk(qbuf.at[1], me - half_first, tok), local_sem.at[5]
        ),
    ]
    for copy in own:
        copy.start()

    barrier = pltpu.get_barrier_semaphore()

    @pl.loop(1, n)
    def _(i):
        pl.semaphore_signal(barrier, inc=1, device_id={"seq": (me + i) % n})

    beside = {"groups": part + 1 - 2 * piece, "seq": me}
    pl.semaphore_signal(barrier, inc=1, device_id=beside)
    pl.semaphore_wait(barrier, n)

    def kv_copies(stage, b, peer, from_hbm):
        slot = b if stage else peer
        return [
            pltpu.make_async_remote_copy(
                src_ref=kvn_hbm if from_hbm else blk(kvn, b, tok),
                dst_ref=blk(kvn, b, tok),
                send_sem=kv_send.at[2 * stage, slot],
                recv_sem=kv_recv.at[0, b],
                device_id={"seq": peer},
            ),
            pltpu.make_async_remote_copy(
                src_ref=kvc_hbm if from_hbm else blk(kvc, b, cac),
                dst_ref=blk(kvc, b, cac),
                send_sem=kv_send.at[2 * stage + 1, slot],
                recv_sem=kv_recv.at[1, b],
                device_id={"seq": peer},
            ),
        ]

    def q_copy(k, peer, source):
        return pltpu.make_async_remote_copy(
            src_ref=cols(q_hbm, (peer + k * half) % n, qw),
            dst_ref=blk(qbuf.at[k], source - half_first, tok),
            send_sem=q_send.at[k, peer],
            recv_sem=q_recv.at[k, source],
            device_id={"seq": peer},
        )

    def o_copy(k, peer, source):
        return pltpu.make_async_remote_copy(
            src_ref=blk(obuf.at[k], peer - half_first, tok),
            dst_ref=cols(out_hbm, (source + k * half) % n, ow),
            send_sem=o_send.at[k, peer],
            recv_sem=o_recv.at[k, source],
            device_id={"seq": peer},
        )

    def own_out(k):
        return pltpu.make_async_copy(
            blk(obuf.at[k], me - half_first, tok),
            cols(out_hbm, (me + k * half) % n, ow),
            own_out_sem.at[k],
        )

    deep = LATENT // chunks

    def w_chunk(which, k, i):
        return weights.at[which, k, pl.ds(pl.multiple_of(i * deep, deep), deep), :]

    def w_direct(i):
        return pltpu.make_async_remote_copy(
            src_ref=w_chunk(piece, 0, i),
            dst_ref=w_chunk(piece, 1, i),
            send_sem=w_send.at[0, i],
            recv_sem=w_recv.at[0, i],
            device_id={"seq": mirror},
        )

    def w_beside(which, i):
        return pltpu.make_async_remote_copy(
            src_ref=w_chunk(which, 1, i),
            dst_ref=w_chunk(which, 1, i),
            send_sem=w_send.at[1, i],
            recv_sem=w_recv.at[1, i],
            device_id=beside,
        )

    @pl.loop(1, slabs)
    def _(j):
        for copy in kv_copies(0, me, exclusive(slab, j, slabs) * INNER + inner, True):
            copy.start()

    near = (inner // 2) * 2
    far = (near + 2) % INNER

    def q_near(k):
        @pl.loop(1, half_slabs)
        def _(j):
            other = exclusive(slab, j, slabs) * INNER
            for c in range(2):
                q_copy(k, other + near + c, me).start()

    def q_slab(k):
        @pl.loop(1, INNER)
        def _(i):
            q_copy(k, slab * INNER + (inner + i) % INNER, me).start()

    def q_far(k):
        @pl.loop(1, half_slabs)
        def _(j):
            other = exclusive(slab, j, slabs) * INNER
            for c in range(2):
                q_copy(k, other + far + c, me).start()

    q_near(0)

    across = slab * INNER + (inner + 2) % INNER
    twin = me + 1 - 2 * (me % 2)
    own[0].wait()
    own[1].wait()

    @pl.loop(0, slabs)
    def _(j):
        b = exclusive(slab, j, slabs) * INNER + inner

        @pl.when(j > 0)
        def _():
            for copy in kv_copies(0, b, twin, False):
                copy.wait_recv()

        for copy in kv_copies(1, b, across, False):
            copy.start()
        for copy in kv_copies(2, b, twin, False):
            copy.start()

    q_slab(0)

    @pl.loop(0, slabs)
    def _(j):
        b = exclusive(slab, j, slabs) * INNER + (inner + 2) % INNER
        for copy in kv_copies(1, b, twin, False):
            copy.wait_recv()
        for copy in kv_copies(2, b, twin, False):
            copy.start()

    q_far(0)
    own[2].wait()
    own[3].wait()

    @pl.loop(0, chunks)
    def _(i):
        w_direct(i).start()

    q_near(1)
    q_slab(1)
    q_far(1)

    csize = math.gcd(C, 256)
    tsize = math.gcd(T, 256)

    @pl.loop(0, T // tsize)
    def _(i):
        first = pl.multiple_of(i * tsize, tsize)
        at = pl.ds(first, tsize)
        lane = lax.broadcasted_iota(jnp.int32, (tsize, 128), 1)
        position = plen_ref[0] + first + lax.broadcasted_iota(jnp.int32, (tsize, 128), 0)
        phase = position.astype(f32) * inverse_ref[...]
        cos_ref[at, :] = jnp.cos(phase)
        sine = jnp.sin(phase)
        sin_ref[at, :] = jnp.where(lane % ROPE < ROPE // 2, -sine, sine)

    @pl.loop(0, slabs)
    def _(j):
        for k in range(2):
            b = exclusive(slab, j, slabs) * INNER + (twin + 2 * k) % INNER
            for copy in kv_copies(2, b, twin, False):
                copy.wait_recv()

    own[4].wait()
    own[5].wait()

    def project(k, latent, rope, first, size):
        lane = lax.broadcasted_iota(jnp.int32, (size, 128), 1)
        at = pl.ds(first, size)
        rope_even = jnp.where(lane < ROPE, rope, 0.0).astype(bf16)
        for h in range(0, heads, 2):
            pair = jnp.dot(latent, weights[0, k, :, h * NOPE : (h + 2) * NOPE], preferred_element_type=f32)
            keys[h, at, 0:128] = pair[:, :128].astype(bf16)
            keys[h, at, 128:256] = rope_even
            turned = pltpu.roll(pair[:, 128:], 64, 1)
            keys[h + 1, at, 0:128] = jnp.where(lane < ROPE, 0.0, turned).astype(bf16)
            keys[h + 1, at, 128:256] = jnp.where(lane < ROPE, turned, rope).astype(bf16)
            vals[at, h * VH : (h + 2) * VH] = jnp.dot(
                latent, weights[1, k, :, h * VH : (h + 2) * VH], preferred_element_type=f32
            ).astype(bf16)

    scale = math.log2(math.e) / math.sqrt(WIDTH)
    per_slab = chunks // half_slabs

    @pl.loop(0, 2)
    def _(k):
        @pl.when(k == 1)
        def _():
            @pl.loop(0, chunks)
            def _(i):
                w_beside(1 - piece, i).wait_recv()

        @pl.loop(0, C // csize)
        def _(i):
            first = pl.multiple_of(i * csize, csize)
            raw = kvc[pl.ds(first, csize), :]
            rope = raw[:, LATENT:].astype(f32)
            project(k, raw[:, :LATENT], jnp.concatenate([rope, rope], 1), first, csize)

        @pl.loop(0, T // tsize)
        def _(i):
            first = pl.multiple_of(i * tsize, tsize)
            at = pl.ds(first, tsize)
            raw = kvn[at, :]
            wide = raw[:, :LATENT].astype(f32)
            inv = lax.rsqrt(jnp.mean(wide * wide, axis=1, keepdims=True) + epsilon)
            latent = (wide * inv * gain_ref[...]).astype(bf16)
            rope = raw[:, LATENT:].astype(f32)
            rope = jnp.concatenate([rope, rope], 1)
            lane = lax.broadcasted_iota(jnp.int32, (tsize, 128), 1)
            rope = rope * cos_ref[at, :] + swap_halves(rope, lane) * sin_ref[at, :]
            project(k, latent, rope, pl.multiple_of(C + first, tsize), tsize)

        @pl.loop(0, half_slabs)
        def _(j):
            group = exclusive(slab, j + k * (half_slabs - 1 - 2 * j), slabs)

            @pl.loop(0, INNER)
            def _(i):
                b = group * INNER + i

                @pl.when(b != me)
                def _():
                    q_copy(k, me, b).wait_recv()

            base = pl.multiple_of(group * rows, rows)
            at = pl.ds(base, rows)
            near_at = pl.ds(pl.multiple_of(base - half_first * tok, rows), rows)
            row = base + lax.broadcasted_iota(jnp.int32, (rows, S), 0)
            col = lax.broadcasted_iota(jnp.int32, (rows, S), 1)
            live = ((col < C) & (col < plen_ref[0])) | ((col >= C) & (col - C <= row))
            bias[...] = jnp.where(live, 0.0, -1e30)

            @pl.loop(0, heads // 2)
            def _(p):
                lane = lax.broadcasted_iota(jnp.int32, (rows, 128), 1)
                cosine = cos_ref[at, :]
                sine = sin_ref[at, :]

                def third(i):
                    return qbuf[k, near_at, pl.ds(pl.multiple_of(p * 384 + 128 * i, 128), 128)]

                def turn(x, hit):
                    x = x.astype(f32)
                    y = x * cosine + swap_halves(x, lane) * sine
                    return jnp.where(hit, y, x).astype(bf16)

                front = third(0)
                middle = turn(third(1), lane < ROPE)
                back = turn(third(2), lane >= ROPE)
                for side, query in enumerate(
                    (jnp.concatenate([front, middle], 1), jnp.concatenate([middle, back], 1))
                ):
                    h = 2 * p + side
                    scores = lax.dot_general(
                        query, keys[h], (((1,), (1,)), ((), ())), preferred_element_type=f32
                    )
                    scores = scores * scale + bias[...]
                    top = jnp.max(scores, axis=1, keepdims=True)
                    grown = jnp.exp2(scores - top)
                    total = jnp.sum(grown, axis=1, keepdims=True)
                    across_v = pl.ds(pl.multiple_of(h * VH, VH), VH)
                    mixed = jnp.dot(grown.astype(bf16), vals[:, across_v], preferred_element_type=f32)
                    obuf[k, near_at, across_v] = (mixed / total).astype(bf16)

            @pl.loop(0, INNER)
            def _(i):
                b = group * INNER + i

                @pl.when(b != me)
                def _():
                    o_copy(k, b, me).start()

                @pl.when(b == me)
                def _():
                    own_out(k).start()

            @pl.when(k == 0)
            def _():
                @pl.loop(j * per_slab, (j + 1) * per_slab)
                def _(i):
                    w_direct(i).wait_recv()
                    w_beside(piece, i).start()

    for k in range(2):
        own_out(k).wait()

        @pl.loop(1, half)
        def _(i):
            peer = half_first + (me + i) % half
            q_copy(k, peer, me).wait_send()
            o_copy(k, peer, me).wait_send()
            o_copy(k, me, peer).wait_recv()

    @pl.loop(0, chunks)
    def _(i):
        w_direct(i).wait_send()
        w_beside(piece, i).wait_send()

    @pl.loop(0, slabs)
    def _(j):
        b = exclusive(slab, j, slabs) * INNER + inner

        @pl.when(j > 0)
        def _():
            for copy in kv_copies(0, me, b, True):
                copy.wait_send()

        for copy in kv_copies(1, b, across, False):
            copy.wait_send()
        for k in range(2):
            d = exclusive(slab, j, slabs) * INNER + (inner + 2 * k) % INNER
            for copy in kv_copies(2, d, twin, False):
                copy.wait_send()


PLANES = 4
EXTRA_END = 2
EXTRA_MIDDLE = 1


def planes_kernel(
    n, tok, cac, heads,
    q_hbm, kvn_hbm, kvc_hbm, wk_hbm, wv_hbm, gain_ref, inverse_ref, plen_ref,
    out_hbm,
    qbuf, kvn, kvc, weights, latents, aux, keys, vals, bias, score_a, score_b, prob_a, prob_b, obuf,
    cos_ref, sin_ref,
    local_sem, own_q_sem, own_out_sem, q_send, q_recv, kv_send, kv_recv, o_send, o_recv, w_send, w_recv,
):
    me = lax.axis_index("seq")
    part = lax.axis_index("groups")
    piece = part % 2
    plane = me // INNER
    inner = me % INNER
    side = plane // (PLANES // 2)
    last = PLANES - 1

    def whole(r):
        return r + side * (last - 2 * r)

    middle = whole(plane)
    end = middle == 0
    mid = middle == 1
    T, C = n * tok, n * cac
    S = T + C
    qw = heads * WIDTH
    ow = heads * VH
    rows = INNER * tok
    pairs = heads // 2
    f32, bf16 = jnp.float32, jnp.bfloat16
    scale = math.log2(math.e) / math.sqrt(WIDTH)

    def blk(ref, b, size):
        return ref.at[pl.ds(pl.multiple_of(b * size, size), size), :]

    def cols(ref, b, size):
        return ref.at[:, pl.ds(pl.multiple_of(b * size, 128), size)]

    def head_plane(k):
        return whole(jnp.where(end, k, jnp.where(k == 0, 1, jnp.where(k == 1, 0, k))))

    steps = 3 + middle

    def own_q(k):
        return pltpu.make_async_copy(
            cols(q_hbm, head_plane(k) * INNER + inner, qw), blk(qbuf.at[k], inner, tok), own_q_sem.at[k]
        )

    own = [
        pltpu.make_async_copy(kvn_hbm, blk(kvn, me, tok), local_sem.at[0]),
        pltpu.make_async_copy(kvc_hbm, blk(kvc, me, cac), local_sem.at[1]),
        pltpu.make_async_copy(wk_hbm, weights.at[0, 0], local_sem.at[2]),
        pltpu.make_async_copy(wv_hbm, weights.at[0, 1], local_sem.at[3]),
    ]
    for copy in own:
        copy.start()

    barrier = pltpu.get_barrier_semaphore()

    @pl.loop(1, n)
    def _(i):
        pl.semaphore_signal(barrier, inc=1, device_id={"seq": (me + i) % n})

    beside = {"groups": part + 1 - 2 * piece, "seq": me}
    pl.semaphore_signal(barrier, inc=1, device_id=beside)
    pl.semaphore_wait(barrier, n)

    def kv_copies(stage, b, peer, from_hbm):
        slot = b if stage else peer
        return [
            pltpu.make_async_remote_copy(
                src_ref=kvn_hbm if from_hbm else blk(kvn, b, tok),
                dst_ref=blk(kvn, b, tok),
                send_sem=kv_send.at[2 * stage, slot],
                recv_sem=kv_recv.at[0, b],
                device_id={"seq": peer},
            ),
            pltpu.make_async_remote_copy(
                src_ref=kvc_hbm if from_hbm else blk(kvc, b, cac),
                dst_ref=blk(kvc, b, cac),
                send_sem=kv_send.at[2 * stage + 1, slot],
                recv_sem=kv_recv.at[1, b],
                device_id={"seq": peer},
            ),
        ]

    def q_copy(k, to_plane, to, source):
        columns = jnp.where(k == PLANES, whole(last), head_plane(k)) * INNER + to
        return pltpu.make_async_remote_copy(
            src_ref=cols(q_hbm, columns, qw),
            dst_ref=blk(qbuf.at[k], source, tok),
            send_sem=q_send.at[k, to],
            recv_sem=q_recv.at[k, source],
            device_id={"seq": to_plane * INNER + to},
        )

    def o_copy(k, to_plane, to, source):
        columns = jnp.where(k == PLANES, whole(last), head_plane(k)) * INNER + source
        return pltpu.make_async_remote_copy(
            src_ref=blk(obuf.at[k], to, tok),
            dst_ref=cols(out_hbm, columns, ow),
            send_sem=o_send.at[k, to],
            recv_sem=o_recv.at[k, source],
            device_id={"seq": to_plane * INNER + to},
        )

    def own_out(k):
        return pltpu.make_async_copy(
            blk(obuf.at[k], inner, tok), cols(out_hbm, head_plane(k) * INNER + inner, ow), own_out_sem.at[k]
        )

    def w_chunk(k, which, i):
        return weights.at[k, which, :, pl.ds(pl.multiple_of(i * 2 * NOPE, 128), 2 * NOPE)]

    def w_copy(way, k, to_k, which, i, device):
        return pltpu.make_async_remote_copy(
            src_ref=w_chunk(k, which, i),
            dst_ref=w_chunk(to_k, which, i),
            send_sem=w_send.at[way, k, which, i],
            recv_sem=w_recv.at[to_k, which, i],
            device_id=device,
        )

    near = {"seq": whole(1 - middle) * INNER + inner}
    beyond = {"seq": whole(2) * INNER + inner}

    def w_near(k, which, i):
        return w_copy(0, k, jnp.where(k == 0, 1, 2), which, i, near)

    def w_beyond(k, which, i):
        return w_copy(1, k, k + 2, which, i, beyond)

    def w_beside(k, i):
        return w_copy(2, k, k, piece, i, beside)

    def extras(k):
        return jnp.where(mid, jnp.where(k == 1, EXTRA_END, jnp.where(k == 2, EXTRA_MIDDLE, 0)), 0)

    def for_own_weights(do):
        @pl.loop(0, pairs)
        def _(i):
            do(w_near(0, piece, i))

            @pl.when(mid)
            def _():
                do(w_beyond(0, piece, i))

        @pl.when(end)
        def _():
            @pl.loop(pairs - EXTRA_END, pairs)
            def _(i):
                do(w_near(0, 1 - piece, i))

        @pl.when(mid)
        def _():
            @pl.loop(pairs - EXTRA_MIDDLE, pairs)
            def _(i):
                do(w_beyond(0, 1 - piece, i))

    def for_forwards(k, i, do):
        @pl.when(mid & (k == 1))
        def _():
            do(w_beyond(k, piece, i))

        @pl.when(mid & (k == 2))
        def _():
            do(w_near(k, piece, i))

        @pl.when(i < pairs - extras(k))
        def _():
            do(w_beside(k, i))

    def pass_on(k, i):
        w_copy(2, k, k, piece, i, beside).wait_recv()
        for_forwards(k, i, lambda copy: copy.start())

    @pl.loop(1, PLANES)
    def _(j):
        for copy in kv_copies(0, me, exclusive(plane, j, PLANES) * INNER + inner, True):
            copy.start()

    own[2].wait()
    own[3].wait()
    for_own_weights(lambda copy: copy.start())

    across = plane * INNER + (inner + 2) % INNER
    twin = me + 1 - 2 * (me % 2)
    own[0].wait()
    own[1].wait()

    @pl.loop(0, steps)
    def _(k):
        own_q(k).start()

    @pl.loop(0, PLANES)
    def _(j):
        b = exclusive(plane, j, PLANES) * INNER + inner

        @pl.when(j > 0)
        def _():
            for copy in kv_copies(0, b, twin, False):
                copy.wait_recv()

        for copy in kv_copies(1, b, across, False):
            copy.start()
        for copy in kv_copies(2, b, twin, False):
            copy.start()

    def for_queries(k, do):
        @pl.loop(1, INNER)
        def _(i):
            do(q_copy(k, plane, (inner + i) % INNER, inner))

    for_queries(0, lambda copy: copy.start())

    tsize = math.gcd(T, 256)
    csize = math.gcd(C, 256)

    @pl.loop(0, T // tsize)
    def _(i):
        first = pl.multiple_of(i * tsize, tsize)
        at = pl.ds(first, tsize)
        lane = lax.broadcasted_iota(jnp.int32, (tsize, 128), 1)
        position = plen_ref[0] + first + lax.broadcasted_iota(jnp.int32, (tsize, 128), 0)
        phase = position.astype(f32) * inverse_ref[...]
        cos_ref[at, :] = jnp.cos(phase)
        sine = jnp.sin(phase)
        sin_ref[at, :] = jnp.where(lane % ROPE < ROPE // 2, -sine, sine)

    bias[...] = jnp.where(
        lax.broadcasted_iota(jnp.int32, (rows, rows), 1) <= lax.broadcasted_iota(jnp.int32, (rows, rows), 0),
        0.0, -1e30,
    )

    @pl.loop(0, PLANES)
    def _(j):
        b = exclusive(plane, j, PLANES) * INNER + (inner + 2) % INNER
        for copy in kv_copies(1, b, twin, False):
            copy.wait_recv()
        for copy in kv_copies(2, b, twin, False):
            copy.start()

    @pl.loop(1, steps)
    def _(k):
        for_queries(k, lambda copy: copy.start())

    def for_far_queries(do):
        @pl.loop(0, INNER)
        def _(i):
            do(q_copy(PLANES, whole(1), (inner + i) % INNER, inner))

    @pl.when(end)
    def _():
        for_far_queries(lambda copy: copy.start())

    @pl.loop(0, heads)
    def _(h):
        vals[h, :, 128:256] = jnp.ones((S, 128), bf16)

    @pl.loop(0, PLANES)
    def _(j):
        for k in range(2):
            b = exclusive(plane, j, PLANES) * INNER + (twin + 2 * k) % INNER
            for copy in kv_copies(2, b, twin, False):
                copy.wait_recv()

    def keep_rope(first, size, rope, dead):
        at = pl.ds(first, size)
        lane = lax.broadcasted_iota(jnp.int32, (size, 128), 1)
        low = lane < ROPE
        aux[at, :] = jnp.where(low, jnp.where(lane == 0, dead, 0.0), rope)
        tail = jnp.where(low, rope, jnp.where(lane == ROPE, dead, 0.0)).astype(bf16)
        for h in range(0, heads, 2):
            keys[h, at, 128:256] = tail

    @pl.loop(0, C // csize)
    def _(i):
        first = pl.multiple_of(i * csize, csize)
        raw = kvc[pl.ds(first, csize), :]
        latents[pl.ds(first, csize), :] = raw[:, :LATENT]
        rope = raw[:, LATENT:].astype(f32)
        row = first + lax.broadcasted_iota(jnp.int32, (csize, 128), 0)
        dead = jnp.where(row < plen_ref[0], 0.0, -1e30)
        keep_rope(first, csize, jnp.concatenate([rope, rope], 1), dead)

    @pl.loop(0, T // tsize)
    def _(i):
        first = pl.multiple_of(i * tsize, tsize)
        at = pl.ds(first, tsize)
        raw = kvn[at, :]
        wide = raw[:, :LATENT].astype(f32)
        inv = lax.rsqrt(jnp.mean(wide * wide, axis=1, keepdims=True) + epsilon)
        latents[pl.ds(pl.multiple_of(C + first, tsize), tsize), :] = (wide * inv * gain_ref[...]).astype(bf16)
        rope = raw[:, LATENT:].astype(f32)
        rope = jnp.concatenate([rope, rope], 1)
        lane = lax.broadcasted_iota(jnp.int32, (tsize, 128), 1)
        rope = rope * cos_ref[at, :] + swap_halves(rope, lane) * sin_ref[at, :]
        keep_rope(pl.multiple_of(C + first, tsize), tsize, rope, 0.0)
        cos_ref[at, :] = cos_ref[at, :] * scale
        sin_ref[at, :] = sin_ref[at, :] * scale

    size = math.gcd(C, rows)

    def project(k, p):
        across_k = pl.ds(pl.multiple_of(p * 2 * NOPE, 128), 2 * NOPE)
        across_v = pl.ds(pl.multiple_of(p * 2 * VH, 128), 2 * VH)

        top_plane = jnp.where(mid & (k == last), jnp.maximum(plane, whole(0)), plane)

        @pl.loop(0, (C + (top_plane + 1) * rows) // size)
        def _(i):
            at = pl.ds(pl.multiple_of(i * size, size), size)
            latent = latents[at, :]
            rest = aux[at, :]
            lane = lax.broadcasted_iota(jnp.int32, (size, 128), 1)
            pair = jnp.dot(latent, weights[k, 0, :, across_k], preferred_element_type=f32) * scale
            keys[2 * p, at, 0:128] = pair[:, :128].astype(bf16)
            turned = pltpu.roll(pair[:, 128:], 64, 1)
            keys[2 * p + 1, at, 0:128] = jnp.where(lane < ROPE, rest, turned).astype(bf16)
            keys[2 * p + 1, at, 128:256] = jnp.where(lane < ROPE, turned, rest).astype(bf16)
            both = jnp.dot(latent, weights[k, 1, :, across_v], preferred_element_type=f32).astype(bf16)
            vals[2 * p, at, 0:128] = both[:, :128]
            vals[2 * p + 1, at, 0:128] = both[:, 128:]

    def attend(slot, first_row, live):
        cut = live - rows

        def rotated(p):
            at = pl.ds(first_row, rows)
            lane = lax.broadcasted_iota(jnp.int32, (rows, 128), 1)
            cosine = cos_ref[at, :]
            sine = sin_ref[at, :]

            def third(i):
                return qbuf[slot, :, pl.ds(pl.multiple_of(p * 3 * 128 + 128 * i, 128), 128)]

            def turn(x, hit):
                x = x.astype(f32)
                y = x * cosine + swap_halves(x, lane) * sine
                return jnp.where(hit, y, x)

            centre = turn(third(1), lane < ROPE)
            return (
                jnp.concatenate([third(0), jnp.where(lane == ROPE, 1.0, centre).astype(bf16)], 1),
                jnp.concatenate(
                    [jnp.where(lane == 0, 1.0, centre).astype(bf16), turn(third(2), lane >= ROPE).astype(bf16)], 1
                ),
            )

        def score(query, h, into):
            into[:, 0:live] = lax.dot_general(
                query, keys[h, 0:live, :], (((1,), (1,)), ((), ())), preferred_element_type=f32
            )

        def soften(scores, into):
            for r in range(0, rows, 16):
                before = scores[r : r + 16, 0:cut]
                near_end = scores[r : r + 16, cut:live] + bias[r : r + 16, :]
                top = jnp.maximum(
                    jnp.max(before, axis=1, keepdims=True), jnp.max(near_end, axis=1, keepdims=True)
                )
                into[r : r + 16, 0:cut] = jnp.exp2(before - top).astype(bf16)
                into[r : r + 16, cut:live] = jnp.exp2(near_end - top).astype(bf16)

        def mix(probs, h):
            mixed = jnp.dot(probs[:, 0:live], vals[h, 0:live, :], preferred_element_type=f32)
            obuf[slot, :, pl.ds(pl.multiple_of(h * VH, VH), VH)] = (mixed[:, :VH] / mixed[:, VH:]).astype(bf16)

        @pl.loop(0, pairs + 1)
        def _(t):
            p = jnp.minimum(t, pairs - 1)
            done = jnp.maximum(t - 1, 0)
            even, odd = rotated(p)
            score(even, 2 * p, score_a)
            soften(score_b, prob_b)
            mix(prob_a, 2 * done)
            soften(score_a, prob_a)
            mix(prob_b, 2 * done + 1)
            score(odd, 2 * p + 1, score_b)

    @pl.loop(0, steps)
    def _(k):
        far = mid & (k == last)

        @pl.loop(0, pairs)
        def _(p):
            @pl.when(k > 0)
            def _():
                @pl.when((k == 1) | (end & (k == 2)) | ((k == 3) & (p >= 2)))
                def _():
                    pass_on(k, p)

                @pl.when(mid & (k == 1))
                def _():
                    pass_on(2, p)

                w_copy(2, k, k, 1 - piece, p, beside).wait_recv()

            project(k, p)

        @pl.when(mid & (k == 2))
        def _():
            pass_on(3, 0)
            pass_on(3, 1)

        own_q(k).wait()

        @pl.loop(1, INNER)
        def _(i):
            q_copy(k, plane, inner, (inner + i) % INNER).wait_recv()

        for s in range(PLANES):
            @pl.when(plane == s)
            def _():
                attend(k, s * rows, C + (s + 1) * rows)

        own_out(k).start()

        @pl.loop(1, INNER)
        def _(i):
            o_copy(k, plane, (inner + i) % INNER, inner).start()

        @pl.when(far)
        def _():
            @pl.loop(0, INNER)
            def _(i):
                q_copy(PLANES, plane, inner, i).wait_recv()

    for s in range(PLANES):
        @pl.when(mid & (whole(0) == s))
        def _():
            attend(PLANES, s * rows, C + (s + 1) * rows)

    def for_far_outputs(do):
        @pl.loop(0, INNER)
        def _(i):
            do(o_copy(PLANES, whole(0), (inner + i) % INNER, inner))

    @pl.when(mid)
    def _():
        for_far_outputs(lambda copy: copy.start())

    @pl.loop(0, steps)
    def _(k):
        own_out(k).wait()
        for_queries(k, lambda copy: copy.wait_send())

        @pl.loop(1, INNER)
        def _(i):
            o_copy(k, plane, (inner + i) % INNER, inner).wait_send()
            o_copy(k, plane, inner, (inner + i) % INNER).wait_recv()

    @pl.when(mid)
    def _():
        for_far_outputs(lambda copy: copy.wait_send())

    @pl.when(end)
    def _():
        for_far_queries(lambda copy: copy.wait_send())

        @pl.loop(0, INNER)
        def _(i):
            o_copy(PLANES, plane, inner, i).wait_recv()

    for_own_weights(lambda copy: copy.wait_send())

    @pl.loop(1, steps)
    def _(k):
        @pl.loop(0, pairs)
        def _(i):
            for_forwards(k, i, lambda copy: copy.wait_send())

    @pl.loop(0, PLANES)
    def _(j):
        b = exclusive(plane, j, PLANES) * INNER + inner

        @pl.when(j > 0)
        def _():
            for copy in kv_copies(0, me, b, True):
                copy.wait_send()

        for copy in kv_copies(1, b, across, False):
            copy.wait_send()
        for k in range(2):
            d = exclusive(plane, j, PLANES) * INNER + (inner + 2 * k) % INNER
            for copy in kv_copies(2, d, twin, False):
                copy.wait_send()


def local_any(n, queries, kv_new, kv_cache, kv_gain, w_key, w_value, prefix_len):
    tok = queries.shape[0]
    cac = kv_cache.shape[0]
    heads = w_key.shape[1] // NOPE
    T, C = n * tok, n * cac
    chunks = max(4, n // (2 * INNER))
    hbm = pl.BlockSpec(memory_space=pl.ANY)
    vmem = pl.BlockSpec(memory_space=pltpu.VMEM)
    bf16 = jnp.bfloat16
    dma = pltpu.SemaphoreType.DMA
    return pl.pallas_call(
        functools.partial(kernel, n, tok, cac, heads, chunks),
        out_shape=jax.ShapeDtypeStruct((tok, n * heads * VH), bf16),
        in_specs=[hbm] * 5 + [vmem] * 2 + [pl.BlockSpec(memory_space=pltpu.SMEM)],
        out_specs=hbm,
        scratch_shapes=[
            pltpu.VMEM((2, T // 2, heads * WIDTH), bf16),
            pltpu.VMEM((T, LATENT + ROPE), bf16),
            pltpu.VMEM((C, LATENT + ROPE), bf16),
            pltpu.VMEM((2, 2, LATENT, heads * NOPE), bf16),
            pltpu.VMEM((heads, C + T, 256), bf16),
            pltpu.VMEM((C + T, heads * VH), bf16),
            pltpu.VMEM((INNER * tok, C + T), jnp.float32),
            pltpu.VMEM((2, T // 2, heads * VH), bf16),
            pltpu.VMEM((T, 128), jnp.float32),
            pltpu.VMEM((T, 128), jnp.float32),
            dma((6,)),
            dma((2,)),
            dma((2, n)),
            dma((2, n)),
            dma((6, n)),
            dma((2, n)),
            dma((2, n)),
            dma((2, n)),
            dma((2, chunks)),
            dma((2, chunks)),
        ],
        compiler_params=pltpu.CompilerParams(
            collective_id=0, has_side_effects=True, vmem_limit_bytes=60 * 2**20
        ),
        name="latent_attention",
    )(queries, kv_new, kv_cache, w_key, w_value, kv_gain[None, :], inverse_lanes(), prefix_len)


def local_planes(n, queries, kv_new, kv_cache, kv_gain, w_key, w_value, prefix_len):
    tok = queries.shape[0]
    cac = kv_cache.shape[0]
    heads = w_key.shape[1] // NOPE
    T, C = n * tok, n * cac
    S = T + C
    rows = INNER * tok
    pairs = heads // 2
    hbm = pl.BlockSpec(memory_space=pl.ANY)
    vmem = pl.BlockSpec(memory_space=pltpu.VMEM)
    bf16, f32 = jnp.bfloat16, jnp.float32
    dma = pltpu.SemaphoreType.DMA
    return pl.pallas_call(
        functools.partial(planes_kernel, n, tok, cac, heads),
        out_shape=jax.ShapeDtypeStruct((tok, n * heads * VH), bf16),
        in_specs=[hbm] * 5 + [vmem] * 2 + [pl.BlockSpec(memory_space=pltpu.SMEM)],
        out_specs=hbm,
        scratch_shapes=[
            pltpu.VMEM((PLANES + 1, rows, heads * WIDTH), bf16),
            pltpu.VMEM((T, LATENT + ROPE), bf16),
            pltpu.VMEM((C, LATENT + ROPE), bf16),
            pltpu.VMEM((PLANES, 2, LATENT, heads * NOPE), bf16),
            pltpu.VMEM((S, LATENT), bf16),
            pltpu.VMEM((S, 128), f32),
            pltpu.VMEM((heads, S, 256), bf16),
            pltpu.VMEM((heads, S, 256), bf16),
            pltpu.VMEM((rows, rows), f32),
            pltpu.VMEM((rows, S), f32),
            pltpu.VMEM((rows, S), f32),
            pltpu.VMEM((rows, S), bf16),
            pltpu.VMEM((rows, S), bf16),
            pltpu.VMEM((PLANES + 1, rows, heads * VH), bf16),
            pltpu.VMEM((T, 128), f32),
            pltpu.VMEM((T, 128), f32),
            dma((4,)),
            dma((PLANES,)),
            dma((PLANES,)),
            dma((PLANES + 1, INNER)),
            dma((PLANES + 1, INNER)),
            dma((6, n)),
            dma((2, n)),
            dma((PLANES + 1, INNER)),
            dma((PLANES + 1, INNER)),
            dma((3, PLANES, 2, pairs)),
            dma((PLANES, 2, pairs)),
        ],
        compiler_params=pltpu.CompilerParams(
            collective_id=0, has_side_effects=True, vmem_limit_bytes=60 * 2**20
        ),
        name="latent_attention",
    )(queries, kv_new, kv_cache, w_key, w_value, kv_gain[None, :], inverse_lanes(), prefix_len)


def local(n, *operands):
    run = local_planes if n == PLANES * INNER else local_any
    return run(n, *operands)


def solution(mesh):
    placed = (
        P(("groups", "seq"), None),
        P(("groups", "seq"), None),
        P(("groups", "seq"), None),
        P(),
        P(None, "seq"),
        P(None, "seq"),
        P("groups"),
    )
    return jax.shard_map(
        functools.partial(local, mesh.shape["seq"]),
        mesh=mesh,
        in_specs=placed,
        out_specs=P(("groups", "seq"), None),
        check_vma=False,
    )
```

```python
import functools
import math

import jax
import jax.numpy as jnp
from jax import lax
from jax.experimental import pallas as pl
from jax.experimental.pallas import tpu as pltpu
from jax.sharding import PartitionSpec as P

NOPE = 128
ROPE = 64
LATENT = 512
VH = 128
WIDTH = NOPE + ROPE
INNER = 4

epsilon = 1e-06


def exclusive(a, b, extent):
    result = 0
    bit = 1
    while bit < extent:
        result = result + ((a // bit + b // bit) % 2) * bit
        bit *= 2
    return result


def inverse_lanes():
    half = ROPE // 2
    inverse = 10000.0 ** (-(jnp.arange(half, dtype=jnp.float32) * 2.0) / ROPE)
    return jnp.concatenate([inverse] * 4)[None, :]


def swap_halves(x, lane):
    return jnp.where(lane % ROPE < ROPE // 2, pltpu.roll(x, 96, 1), pltpu.roll(x, 32, 1))


def kernel(
    n, tok, cac, heads, chunks,
    q_hbm, kvn_hbm, kvc_hbm, wk_hbm, wv_hbm, gain_ref, inverse_ref, plen_ref,
    out_hbm,
    qbuf, kvn, kvc, weights, keys, vals, bias, obuf, cos_ref, sin_ref,
    local_sem, own_out_sem, q_send, q_recv, kv_send, kv_recv, o_send, o_recv, w_send, w_recv,
):
    me = lax.axis_index("seq")
    part = lax.axis_index("groups")
    piece = part % 2
    half = n // 2
    mirror = (me + half) % n
    half_first = (me // half) * half
    half_slabs = half // INNER
    slab = me // INNER
    inner = me % INNER
    slabs = n // INNER
    T, C = n * tok, n * cac
    S = T + C
    qw = heads * WIDTH
    ow = heads * VH
    rows = INNER * tok
    f32, bf16 = jnp.float32, jnp.bfloat16

    def blk(ref, b, size):
        return ref.at[pl.ds(pl.multiple_of(b * size, size), size), :]

    def cols(ref, b, size):
        return ref.at[:, pl.ds(pl.multiple_of(b * size, 128), size)]

    own = [
        pltpu.make_async_copy(kvn_hbm, blk(kvn, me, tok), local_sem.at[0]),
        pltpu.make_async_copy(kvc_hbm, blk(kvc, me, cac), local_sem.at[1]),
        pltpu.make_async_copy(wk_hbm, weights.at[0, 0], local_sem.at[2]),
        pltpu.make_async_copy(wv_hbm, weights.at[1, 0], local_sem.at[3]),
        pltpu.make_async_copy(
            cols(q_hbm, me, qw), blk(qbuf.at[0], me - half_first, tok), local_sem.at[4]
        ),
        pltpu.make_async_copy(
            cols(q_hbm, mirror, qw), blk(qbuf.at[1], me - half_first, tok), local_sem.at[5]
        ),
    ]
    for copy in own:
        copy.start()

    barrier = pltpu.get_barrier_semaphore()

    @pl.loop(1, n)
    def _(i):
        pl.semaphore_signal(barrier, inc=1, device_id={"seq": (me + i) % n})

    beside = {"groups": part + 1 - 2 * piece, "seq": me}
    pl.semaphore_signal(barrier, inc=1, device_id=beside)
    pl.semaphore_wait(barrier, n)

    def kv_copies(stage, b, peer, from_hbm):
        slot = b if stage else peer
        return [
            pltpu.make_async_remote_copy(
                src_ref=kvn_hbm if from_hbm else blk(kvn, b, tok),
                dst_ref=blk(kvn, b, tok),
                send_sem=kv_send.at[2 * stage, slot],
                recv_sem=kv_recv.at[0, b],
                device_id={"seq": peer},
            ),
            pltpu.make_async_remote_copy(
                src_ref=kvc_hbm if from_hbm else blk(kvc, b, cac),
                dst_ref=blk(kvc, b, cac),
                send_sem=kv_send.at[2 * stage + 1, slot],
                recv_sem=kv_recv.at[1, b],
                device_id={"seq": peer},
            ),
        ]

    def q_copy(k, peer, source):
        return pltpu.make_async_remote_copy(
            src_ref=cols(q_hbm, (peer + k * half) % n, qw),
            dst_ref=blk(qbuf.at[k], source - half_first, tok),
            send_sem=q_send.at[k, peer],
            recv_sem=q_recv.at[k, source],
            device_id={"seq": peer},
        )

    def o_copy(k, peer, source):
        return pltpu.make_async_remote_copy(
            src_ref=blk(obuf.at[k], peer - half_first, tok),
            dst_ref=cols(out_hbm, (source + k * half) % n, ow),
            send_sem=o_send.at[k, peer],
            recv_sem=o_recv.at[k, source],
            device_id={"seq": peer},
        )

    def own_out(k):
        return pltpu.make_async_copy(
            blk(obuf.at[k], me - half_first, tok),
            cols(out_hbm, (me + k * half) % n, ow),
            own_out_sem.at[k],
        )

    deep = LATENT // chunks

    def w_chunk(which, k, i):
        return weights.at[which, k, pl.ds(pl.multiple_of(i * deep, deep), deep), :]

    def w_direct(i):
        return pltpu.make_async_remote_copy(
            src_ref=w_chunk(piece, 0, i),
            dst_ref=w_chunk(piece, 1, i),
            send_sem=w_send.at[0, i],
            recv_sem=w_recv.at[0, i],
            device_id={"seq": mirror},
        )

    def w_beside(which, i):
        return pltpu.make_async_remote_copy(
            src_ref=w_chunk(which, 1, i),
            dst_ref=w_chunk(which, 1, i),
            send_sem=w_send.at[1, i],
            recv_sem=w_recv.at[1, i],
            device_id=beside,
        )

    @pl.loop(1, slabs)
    def _(j):
        for copy in kv_copies(0, me, exclusive(slab, j, slabs) * INNER + inner, True):
            copy.start()

    near = (inner // 2) * 2
    far = (near + 2) % INNER

    def q_near(k):
        @pl.loop(1, half_slabs)
        def _(j):
            other = exclusive(slab, j, slabs) * INNER
            for c in range(2):
                q_copy(k, other + near + c, me).start()

    def q_slab(k):
        @pl.loop(1, INNER)
        def _(i):
            q_copy(k, slab * INNER + (inner + i) % INNER, me).start()

    def q_far(k):
        @pl.loop(1, half_slabs)
        def _(j):
            other = exclusive(slab, j, slabs) * INNER
            for c in range(2):
                q_copy(k, other + far + c, me).start()

    q_near(0)

    across = slab * INNER + (inner + 2) % INNER
    twin = me + 1 - 2 * (me % 2)
    own[0].wait()
    own[1].wait()

    @pl.loop(0, slabs)
    def _(j):
        b = exclusive(slab, j, slabs) * INNER + inner

        @pl.when(j > 0)
        def _():
            for copy in kv_copies(0, b, twin, False):
                copy.wait_recv()

        for copy in kv_copies(1, b, across, False):
            copy.start()
        for copy in kv_copies(2, b, twin, False):
            copy.start()

    q_slab(0)

    @pl.loop(0, slabs)
    def _(j):
        b = exclusive(slab, j, slabs) * INNER + (inner + 2) % INNER
        for copy in kv_copies(1, b, twin, False):
            copy.wait_recv()
        for copy in kv_copies(2, b, twin, False):
            copy.start()

    q_far(0)
    own[2].wait()
    own[3].wait()

    @pl.loop(0, chunks)
    def _(i):
        w_direct(i).start()

    q_near(1)
    q_slab(1)
    q_far(1)

    csize = math.gcd(C, 256)
    tsize = math.gcd(T, 256)

    @pl.loop(0, T // tsize)
    def _(i):
        first = pl.multiple_of(i * tsize, tsize)
        at = pl.ds(first, tsize)
        lane = lax.broadcasted_iota(jnp.int32, (tsize, 128), 1)
        position = plen_ref[0] + first + lax.broadcasted_iota(jnp.int32, (tsize, 128), 0)
        phase = position.astype(f32) * inverse_ref[...]
        cos_ref[at, :] = jnp.cos(phase)
        sine = jnp.sin(phase)
        sin_ref[at, :] = jnp.where(lane % ROPE < ROPE // 2, -sine, sine)

    @pl.loop(0, slabs)
    def _(j):
        for k in range(2):
            b = exclusive(slab, j, slabs) * INNER + (twin + 2 * k) % INNER
            for copy in kv_copies(2, b, twin, False):
                copy.wait_recv()

    own[4].wait()
    own[5].wait()

    def project(k, latent, rope, first, size):
        lane = lax.broadcasted_iota(jnp.int32, (size, 128), 1)
        at = pl.ds(first, size)
        rope_even = jnp.where(lane < ROPE, rope, 0.0).astype(bf16)
        for h in range(0, heads, 2):
            pair = jnp.dot(latent, weights[0, k, :, h * NOPE : (h + 2) * NOPE], preferred_element_type=f32)
            keys[h, at, 0:128] = pair[:, :128].astype(bf16)
            keys[h, at, 128:256] = rope_even
            turned = pltpu.roll(pair[:, 128:], 64, 1)
            keys[h + 1, at, 0:128] = jnp.where(lane < ROPE, 0.0, turned).astype(bf16)
            keys[h + 1, at, 128:256] = jnp.where(lane < ROPE, turned, rope).astype(bf16)
            vals[at, h * VH : (h + 2) * VH] = jnp.dot(
                latent, weights[1, k, :, h * VH : (h + 2) * VH], preferred_element_type=f32
            ).astype(bf16)

    scale = math.log2(math.e) / math.sqrt(WIDTH)
    per_slab = chunks // half_slabs

    @pl.loop(0, 2)
    def _(k):
        @pl.when(k == 1)
        def _():
            @pl.loop(0, chunks)
            def _(i):
                w_beside(1 - piece, i).wait_recv()

        @pl.loop(0, C // csize)
        def _(i):
            first = pl.multiple_of(i * csize, csize)
            raw = kvc[pl.ds(first, csize), :]
            rope = raw[:, LATENT:].astype(f32)
            project(k, raw[:, :LATENT], jnp.concatenate([rope, rope], 1), first, csize)

        @pl.loop(0, T // tsize)
        def _(i):
            first = pl.multiple_of(i * tsize, tsize)
            at = pl.ds(first, tsize)
            raw = kvn[at, :]
            wide = raw[:, :LATENT].astype(f32)
            inv = lax.rsqrt(jnp.mean(wide * wide, axis=1, keepdims=True) + epsilon)
            latent = (wide * inv * gain_ref[...]).astype(bf16)
            rope = raw[:, LATENT:].astype(f32)
            rope = jnp.concatenate([rope, rope], 1)
            lane = lax.broadcasted_iota(jnp.int32, (tsize, 128), 1)
            rope = rope * cos_ref[at, :] + swap_halves(rope, lane) * sin_ref[at, :]
            project(k, latent, rope, pl.multiple_of(C + first, tsize), tsize)

        @pl.loop(0, half_slabs)
        def _(j):
            group = exclusive(slab, j + k * (half_slabs - 1 - 2 * j), slabs)

            @pl.loop(0, INNER)
            def _(i):
                b = group * INNER + i

                @pl.when(b != me)
                def _():
                    q_copy(k, me, b).wait_recv()

            base = pl.multiple_of(group * rows, rows)
            at = pl.ds(base, rows)
            near_at = pl.ds(pl.multiple_of(base - half_first * tok, rows), rows)
            row = base + lax.broadcasted_iota(jnp.int32, (rows, S), 0)
            col = lax.broadcasted_iota(jnp.int32, (rows, S), 1)
            live = ((col < C) & (col < plen_ref[0])) | ((col >= C) & (col - C <= row))
            bias[...] = jnp.where(live, 0.0, -1e30)

            @pl.loop(0, heads // 2)
            def _(p):
                lane = lax.broadcasted_iota(jnp.int32, (rows, 128), 1)
                cosine = cos_ref[at, :]
                sine = sin_ref[at, :]

                def third(i):
                    return qbuf[k, near_at, pl.ds(pl.multiple_of(p * 384 + 128 * i, 128), 128)]

                def turn(x, hit):
                    x = x.astype(f32)
                    y = x * cosine + swap_halves(x, lane) * sine
                    return jnp.where(hit, y, x).astype(bf16)

                front = third(0)
                middle = turn(third(1), lane < ROPE)
                back = turn(third(2), lane >= ROPE)
                for side, query in enumerate(
                    (jnp.concatenate([front, middle], 1), jnp.concatenate([middle, back], 1))
                ):
                    h = 2 * p + side
                    scores = lax.dot_general(
                        query, keys[h], (((1,), (1,)), ((), ())), preferred_element_type=f32
                    )
                    scores = scores * scale + bias[...]
                    top = jnp.max(scores, axis=1, keepdims=True)
                    grown = jnp.exp2(scores - top)
                    total = jnp.sum(grown, axis=1, keepdims=True)
                    across_v = pl.ds(pl.multiple_of(h * VH, VH), VH)
                    mixed = jnp.dot(grown.astype(bf16), vals[:, across_v], preferred_element_type=f32)
                    obuf[k, near_at, across_v] = (mixed / total).astype(bf16)

            @pl.loop(0, INNER)
            def _(i):
                b = group * INNER + i

                @pl.when(b != me)
                def _():
                    o_copy(k, b, me).start()

                @pl.when(b == me)
                def _():
                    own_out(k).start()

            @pl.when(k == 0)
            def _():
                @pl.loop(j * per_slab, (j + 1) * per_slab)
                def _(i):
                    w_direct(i).wait_recv()
                    w_beside(piece, i).start()

    for k in range(2):
        own_out(k).wait()

        @pl.loop(1, half)
        def _(i):
            peer = half_first + (me + i) % half
            q_copy(k, peer, me).wait_send()
            o_copy(k, peer, me).wait_send()
            o_copy(k, me, peer).wait_recv()

    @pl.loop(0, chunks)
    def _(i):
        w_direct(i).wait_send()
        w_beside(piece, i).wait_send()

    @pl.loop(0, slabs)
    def _(j):
        b = exclusive(slab, j, slabs) * INNER + inner

        @pl.when(j > 0)
        def _():
            for copy in kv_copies(0, me, b, True):
                copy.wait_send()

        for copy in kv_copies(1, b, across, False):
            copy.wait_send()
        for k in range(2):
            d = exclusive(slab, j, slabs) * INNER + (inner + 2 * k) % INNER
            for copy in kv_copies(2, d, twin, False):
                copy.wait_send()


PLANES = 4
EXTRA_END = 3
EXTRA_MIDDLE = 0
EXTRA_FAR = 1


def planes_kernel(
    n, tok, cac, heads,
    q_hbm, kvn_hbm, kvc_hbm, wk_hbm, wv_hbm, gain_ref, inverse_ref, plen_ref,
    out_hbm,
    qbuf, kvn, kvc, weights, latents, aux, keys, vals, bias, score_a, score_b, prob_a, prob_b, obuf,
    cos_ref, sin_ref,
    local_sem, own_w_sem, own_q_sem, own_out_sem, q_send, q_recv, kv_send, kv_recv, o_send, o_recv, w_send, w_recv,
):
    me = lax.axis_index("seq")
    part = lax.axis_index("groups")
    piece = part % 2
    plane = me // INNER
    inner = me % INNER
    side = plane // (PLANES // 2)
    last = PLANES - 1

    def whole(r):
        return r + side * (last - 2 * r)

    middle = whole(plane)
    end = middle == 0
    mid = middle == 1
    T, C = n * tok, n * cac
    S = T + C
    qw = heads * WIDTH
    ow = heads * VH
    rows = INNER * tok
    pairs = heads // 2
    f32, bf16 = jnp.float32, jnp.bfloat16
    scale = math.log2(math.e) / math.sqrt(WIDTH)

    def blk(ref, b, size):
        return ref.at[pl.ds(pl.multiple_of(b * size, size), size), :]

    def cols(ref, b, size):
        return ref.at[:, pl.ds(pl.multiple_of(b * size, 128), size)]

    def head_plane(k):
        return whole(jnp.where(end, k, jnp.where(k == 0, 1, jnp.where(k == 1, 0, k))))

    steps = 3 + middle

    def own_q(k):
        return pltpu.make_async_copy(
            cols(q_hbm, head_plane(k) * INNER + inner, qw), blk(qbuf.at[k], inner, tok), own_q_sem.at[k]
        )

    own = [
        pltpu.make_async_copy(kvn_hbm, blk(kvn, me, tok), local_sem.at[0]),
        pltpu.make_async_copy(kvc_hbm, blk(kvc, me, cac), local_sem.at[1]),
    ]
    for copy in own:
        copy.start()

    def own_w(which, i):
        source = wv_hbm if which else wk_hbm
        return pltpu.make_async_copy(cols(source, i, 2 * NOPE), weights.at[0, which, i], own_w_sem.at[which, i])

    for which in range(2):
        @pl.loop(0, pairs)
        def _(i):
            own_w(which, i).start()

    barrier = pltpu.get_barrier_semaphore()

    @pl.loop(1, n)
    def _(i):
        pl.semaphore_signal(barrier, inc=1, device_id={"seq": (me + i) % n})

    beside = {"groups": part + 1 - 2 * piece, "seq": me}
    pl.semaphore_signal(barrier, inc=1, device_id=beside)
    pl.semaphore_wait(barrier, n)

    def kv_copies(stage, b, peer, from_hbm):
        slot = b if stage else peer
        return [
            pltpu.make_async_remote_copy(
                src_ref=kvn_hbm if from_hbm else blk(kvn, b, tok),
                dst_ref=blk(kvn, b, tok),
                send_sem=kv_send.at[2 * stage, slot],
                recv_sem=kv_recv.at[0, b],
                device_id={"seq": peer},
            ),
            pltpu.make_async_remote_copy(
                src_ref=kvc_hbm if from_hbm else blk(kvc, b, cac),
                dst_ref=blk(kvc, b, cac),
                send_sem=kv_send.at[2 * stage + 1, slot],
                recv_sem=kv_recv.at[1, b],
                device_id={"seq": peer},
            ),
        ]

    near = {"seq": whole(1 - middle) * INNER + inner}
    beyond = {"seq": whole(2) * INNER + inner}

    def far_query(source):
        return pltpu.make_async_remote_copy(
            src_ref=blk(qbuf.at[PLANES], source, tok),
            dst_ref=blk(qbuf.at[PLANES], source, tok),
            send_sem=q_send.at[PLANES + 1, source],
            recv_sem=q_recv.at[PLANES, source],
            device_id=near,
        )

    def q_copy(k, to_plane, to, source):
        columns = jnp.where(k == PLANES, whole(last), head_plane(k)) * INNER + to
        return pltpu.make_async_remote_copy(
            src_ref=cols(q_hbm, columns, qw),
            dst_ref=blk(qbuf.at[k], source, tok),
            send_sem=q_send.at[k, to],
            recv_sem=q_recv.at[k, source],
            device_id={"seq": to_plane * INNER + to},
        )

    def o_part(k, part_of, to):
        return obuf.at[k, pl.ds(pl.multiple_of(to * tok, tok), tok), pl.ds(pl.multiple_of(part_of * ow // 2, 128), ow // 2)]

    def o_copy(k, part_of, to_plane, to, source):
        columns = jnp.where(k == PLANES, whole(last), head_plane(k)) * INNER + source
        return pltpu.make_async_remote_copy(
            src_ref=o_part(k, part_of, to),
            dst_ref=cols(out_hbm, 2 * columns + part_of, ow // 2),
            send_sem=o_send.at[k, part_of, to],
            recv_sem=o_recv.at[k, part_of, source],
            device_id={"seq": to_plane * INNER + to},
        )

    def own_out(k, part_of):
        columns = head_plane(k) * INNER + inner
        return pltpu.make_async_copy(
            o_part(k, part_of, inner), cols(out_hbm, 2 * columns + part_of, ow // 2), own_out_sem.at[k, part_of]
        )

    def w_chunk(k, which, i):
        return weights.at[k, which, i]

    def w_copy(way, k, to_k, which, i, device):
        return pltpu.make_async_remote_copy(
            src_ref=w_chunk(k, which, i),
            dst_ref=w_chunk(to_k, which, i),
            send_sem=w_send.at[way, k, which, i],
            recv_sem=w_recv.at[to_k, which, i],
            device_id=device,
        )

    def w_near(k, which, i):
        return w_copy(0, k, jnp.where(k == 0, 1, 2), which, i, near)

    def w_beyond(k, which, i):
        return w_copy(1, k, k + 2, which, i, beyond)

    def w_beside(k, i):
        return w_copy(2, k, k, piece, i, beside)

    def extras(k):
        return jnp.where(mid, jnp.where(k == 1, EXTRA_END, jnp.where(k == 2, EXTRA_MIDDLE, EXTRA_FAR)), 0)

    def for_own_weights(do):
        @pl.loop(0, pairs)
        def _(i):
            do(w_near(0, piece, i))

            @pl.when(mid)
            def _():
                do(w_beyond(0, piece, i))

        @pl.when(end)
        def _():
            @pl.loop(pairs - EXTRA_END, pairs)
            def _(i):
                do(w_near(0, 1 - piece, i))

        @pl.when(mid)
        def _():
            @pl.loop(pairs - EXTRA_MIDDLE, pairs)
            def _(i):
                do(w_beyond(0, 1 - piece, i))

    def for_forwards(k, i, do):
        @pl.when(mid & (k == 1))
        def _():
            do(w_beyond(k, piece, i))

        @pl.when(mid & (k == 2))
        def _():
            do(w_near(k, piece, i))

        @pl.when(i < pairs - extras(k))
        def _():
            do(w_beside(k, i))

    def pass_on(k, i):
        w_copy(2, k, k, piece, i, beside).wait_recv()
        for_forwards(k, i, lambda copy: copy.start())

    @pl.loop(1, PLANES)
    def _(j):
        for copy in kv_copies(0, me, exclusive(plane, j, PLANES) * INNER + inner, True):
            copy.start()

    for which in range(2):
        @pl.loop(0, pairs)
        def _(i):
            own_w(which, i).wait()

    for_own_weights(lambda copy: copy.start())

    across = plane * INNER + (inner + 2) % INNER
    twin = me + 1 - 2 * (me % 2)
    own[0].wait()
    own[1].wait()

    own_far_q = pltpu.make_async_copy(
        cols(q_hbm, whole(last) * INNER + inner, qw), blk(qbuf.at[PLANES], inner, tok), local_sem.at[2]
    )

    @pl.when(end)
    def _():
        own_far_q.start()

    @pl.loop(0, steps)
    def _(k):
        own_q(k).start()

    def for_queries(k, do):
        @pl.loop(1, INNER)
        def _(i):
            do(q_copy(k, plane, (inner + i) % INNER, inner))

    def relay_kv(j):
        b = exclusive(plane, j, PLANES) * INNER + inner
        for copy in kv_copies(1, b, across, False):
            copy.start()
        for copy in kv_copies(2, b, twin, False):
            copy.start()

    relay_kv(0)
    for_queries(0, lambda copy: copy.start())

    @pl.loop(1, PLANES)
    def _(j):
        for copy in kv_copies(0, exclusive(plane, j, PLANES) * INNER + inner, twin, False):
            copy.wait_recv()
        relay_kv(j)

    for_queries(1, lambda copy: copy.start())

    @pl.when(end)
    def _():
        for_queries(PLANES, lambda copy: copy.start())

    @pl.loop(2, steps)
    def _(k):
        for_queries(k, lambda copy: copy.start())

    tsize = math.gcd(T, 256)
    csize = math.gcd(C, 256)

    @pl.loop(0, T // tsize)
    def _(i):
        first = pl.multiple_of(i * tsize, tsize)
        at = pl.ds(first, tsize)
        lane = lax.broadcasted_iota(jnp.int32, (tsize, 128), 1)
        position = plen_ref[0] + first + lax.broadcasted_iota(jnp.int32, (tsize, 128), 0)
        phase = position.astype(f32) * inverse_ref[...]
        cos_ref[at, :] = jnp.cos(phase)
        sine = jnp.sin(phase)
        sin_ref[at, :] = jnp.where(lane % ROPE < ROPE // 2, -sine, sine)

    bias[...] = jnp.where(
        lax.broadcasted_iota(jnp.int32, (rows, rows), 1) <= lax.broadcasted_iota(jnp.int32, (rows, rows), 0),
        0.0, -1e30,
    )

    def pass_on_near(i):
        pass_on(1, i)

        @pl.when(mid)
        def _():
            pass_on(2, i)

    pass_on_near(0)

    @pl.loop(0, PLANES)
    def _(j):
        b = exclusive(plane, j, PLANES) * INNER + (inner + 2) % INNER
        for copy in kv_copies(1, b, twin, False):
            copy.wait_recv()
        for copy in kv_copies(2, b, twin, False):
            copy.start()

    pass_on_near(1)

    @pl.loop(0, heads)
    def _(h):
        vals[h, :, 128:256] = jnp.ones((S, 128), bf16)

    @pl.loop(0, PLANES)
    def _(j):
        for k in range(2):
            b = exclusive(plane, j, PLANES) * INNER + (twin + 2 * k) % INNER
            for copy in kv_copies(2, b, twin, False):
                copy.wait_recv()

    def keep_rope(first, size, rope, dead):
        at = pl.ds(first, size)
        lane = lax.broadcasted_iota(jnp.int32, (size, 128), 1)
        low = lane < ROPE
        aux[at, :] = jnp.where(low, jnp.where(lane == 0, dead, 0.0), rope)
        tail = jnp.where(low, rope, jnp.where(lane == ROPE, dead, 0.0)).astype(bf16)
        for h in range(0, heads, 2):
            keys[h, at, 128:256] = tail

    @pl.loop(0, C // csize)
    def _(i):
        first = pl.multiple_of(i * csize, csize)
        raw = kvc[pl.ds(first, csize), :]
        latents[pl.ds(first, csize), :] = raw[:, :LATENT]
        rope = raw[:, LATENT:].astype(f32)
        row = first + lax.broadcasted_iota(jnp.int32, (csize, 128), 0)
        dead = jnp.where(row < plen_ref[0], 0.0, -1e30)
        keep_rope(first, csize, jnp.concatenate([rope, rope], 1), dead)

    @pl.loop(0, T // tsize)
    def _(i):
        first = pl.multiple_of(i * tsize, tsize)
        at = pl.ds(first, tsize)
        raw = kvn[at, :]
        wide = raw[:, :LATENT].astype(f32)
        inv = lax.rsqrt(jnp.mean(wide * wide, axis=1, keepdims=True) + epsilon)
        latents[pl.ds(pl.multiple_of(C + first, tsize), tsize), :] = (wide * inv * gain_ref[...]).astype(bf16)
        rope = raw[:, LATENT:].astype(f32)
        rope = jnp.concatenate([rope, rope], 1)
        lane = lax.broadcasted_iota(jnp.int32, (tsize, 128), 1)
        rope = rope * cos_ref[at, :] + swap_halves(rope, lane) * sin_ref[at, :]
        keep_rope(pl.multiple_of(C + first, tsize), tsize, rope, 0.0)
        cos_ref[at, :] = cos_ref[at, :] * scale
        sin_ref[at, :] = sin_ref[at, :] * scale

    pass_on_near(2)
    size = math.gcd(C, rows)

    def project_rows(k, p, live):
        lane = lax.broadcasted_iota(jnp.int32, (size, 128), 1)
        for first in range(0, live, size):
            at = slice(first, first + size)
            latent = latents[at, :]
            rest = aux[at, :]
            pair = jnp.dot(latent, weights[k, 0, p], preferred_element_type=f32) * scale
            keys[2 * p, at, 0:128] = pair[:, :128].astype(bf16)
            turned = pltpu.roll(pair[:, 128:], 64, 1)
            keys[2 * p + 1, at, 0:128] = jnp.where(lane < ROPE, rest, turned).astype(bf16)
            keys[2 * p + 1, at, 128:256] = jnp.where(lane < ROPE, turned, rest).astype(bf16)
            both = jnp.dot(latent, weights[k, 1, p], preferred_element_type=f32).astype(bf16)
            vals[2 * p, at, 0:128] = both[:, :128]
            vals[2 * p + 1, at, 0:128] = both[:, 128:]

    def project(k, p):
        top_plane = jnp.where(mid & (k == last), jnp.maximum(plane, whole(0)), plane)
        for s in range(PLANES):
            @pl.when(top_plane == s)
            def _():
                project_rows(k, p, C + (s + 1) * rows)

    def attend(slot, first_row, live, first_pair, last_pair):
        cut = live - rows

        def rotated(p):
            at = pl.ds(first_row, rows)
            lane = lax.broadcasted_iota(jnp.int32, (rows, 128), 1)
            cosine = cos_ref[at, :]
            sine = sin_ref[at, :]

            def third(i):
                return qbuf[slot, :, pl.ds(pl.multiple_of(p * 3 * 128 + 128 * i, 128), 128)]

            def turn(x, hit):
                x = x.astype(f32)
                y = x * cosine + swap_halves(x, lane) * sine
                return jnp.where(hit, y, x)

            centre = turn(third(1), lane < ROPE)
            return (
                jnp.concatenate([third(0), jnp.where(lane == ROPE, 1.0, centre).astype(bf16)], 1),
                jnp.concatenate(
                    [jnp.where(lane == 0, 1.0, centre).astype(bf16), turn(third(2), lane >= ROPE).astype(bf16)], 1
                ),
            )

        def score(query, h, into):
            into[:, 0:live] = lax.dot_general(
                query, keys[h, 0:live, :], (((1,), (1,)), ((), ())), preferred_element_type=f32
            )

        def soften(scores, into):
            for r in range(0, rows, 16):
                before = scores[r : r + 16, 0:cut]
                near_end = scores[r : r + 16, cut:live] + bias[r : r + 16, :]
                top = jnp.maximum(
                    jnp.max(before, axis=1, keepdims=True), jnp.max(near_end, axis=1, keepdims=True)
                )
                into[r : r + 16, 0:cut] = jnp.exp2(before - top).astype(bf16)
                into[r : r + 16, cut:live] = jnp.exp2(near_end - top).astype(bf16)

        def mix(probs, h):
            mixed = jnp.dot(probs[:, 0:live], vals[h, 0:live, :], preferred_element_type=f32)
            obuf[slot, :, pl.ds(pl.multiple_of(h * VH, VH), VH)] = (mixed[:, :VH] / mixed[:, VH:]).astype(bf16)

        @pl.loop(first_pair, last_pair)
        def _(p):
            done = jnp.maximum(p - 1, first_pair)
            even, odd = rotated(p)
            score(even, 2 * p, score_a)
            soften(score_b, prob_b)
            mix(prob_a, 2 * done)
            soften(score_a, prob_a)
            mix(prob_b, 2 * done + 1)
            score(odd, 2 * p + 1, score_b)

        soften(score_b, prob_b)
        mix(prob_a, 2 * last_pair - 2)
        mix(prob_b, 2 * last_pair - 1)

    def attend_plane(slot, s, first_pair, last_pair):
        for plane_of in range(PLANES):
            @pl.when(s == plane_of)
            def _():
                attend(slot, plane_of * rows, C + (plane_of + 1) * rows, first_pair, last_pair)

    def other_kind(k, p):
        w_copy(2, k, k, 1 - piece, p, beside).wait_recv()

        @pl.when(mid & (k == 1) & (p >= pairs - EXTRA_FAR))
        def _():
            w_beyond(k, 1 - piece, p).start()

    @pl.loop(0, jnp.where(end, 5, 7))
    def _(turn):
        j = turn - 1
        late = j >= 4
        k = jnp.where(turn == 0, 0, jnp.where(end, 1 + j // 2, jnp.where(late, last, 2 - j % 2)))
        half = jnp.where(turn == 0, 0, jnp.where(end | late, j % 2, j // 2))
        far = mid & (k == last)
        first_pair = half * (pairs // 2)
        last_pair = jnp.where(turn == 0, pairs, first_pair + pairs // 2)

        @pl.loop(first_pair, last_pair)
        def _(p):
            @pl.when(k > 0)
            def _():
                other_kind(k, p)

            project(k, p)

        @pl.when(half == 0)
        def _():
            own_q(k).wait()

            @pl.loop(1, INNER)
            def _(i):
                q_copy(k, plane, inner, (inner + i) % INNER).wait_recv()

            @pl.when(far)
            def _():
                @pl.loop(0, INNER)
                def _(i):
                    far_query(i).wait_recv()

        @pl.when(end & (turn == 3))
        def _():
            pass_on(2, 2)

        @pl.loop(jnp.where(far, 0, 1), 2)
        def _(item):
            slot = jnp.where(item == 0, PLANES, k)
            attend_plane(slot, jnp.where(item == 0, whole(0), plane), first_pair, last_pair)

            @pl.loop(first_pair // (pairs // 2), last_pair // (pairs // 2))
            def _(part_of):
                @pl.when(item == 0)
                def _():
                    @pl.loop(0, INNER)
                    def _(i):
                        o_copy(PLANES, part_of, whole(0), (inner + i) % INNER, inner).start()

                @pl.when(item == 1)
                def _():
                    own_out(k, part_of).start()

                    @pl.loop(1, INNER)
                    def _(i):
                        o_copy(k, part_of, plane, (inner + i) % INNER, inner).start()

            @pl.when((item == 0) & (turn == 5))
            def _():
                pass_on(3, 3)

        @pl.when(turn == 0)
        def _():
            pass_on_near(3)

        @pl.when(end & (turn > 0) & (turn < 4))
        def _():
            pass_on(2, jnp.where(turn == 3, 3, turn - 1))

        @pl.when(mid & ((turn == 1) | (turn == 3) | (turn == 4)))
        def _():
            pass_on(3, turn // 2)

        @pl.when(end & (turn == 1))
        def _():
            @pl.loop(1, INNER)
            def _(i):
                q_copy(PLANES, plane, inner, (inner + i) % INNER).wait_recv()

            own_far_q.wait()

            @pl.loop(0, INNER)
            def _(i):
                far_query(i).start()

    @pl.loop(0, 2)
    def _(part_of):
        @pl.loop(0, steps)
        def _(k):
            own_out(k, part_of).wait()

            @pl.loop(1, INNER)
            def _(i):
                o_copy(k, part_of, plane, (inner + i) % INNER, inner).wait_send()
                o_copy(k, part_of, plane, inner, (inner + i) % INNER).wait_recv()

        @pl.when(mid)
        def _():
            @pl.loop(0, INNER)
            def _(i):
                o_copy(PLANES, part_of, whole(0), (inner + i) % INNER, inner).wait_send()

        @pl.when(end)
        def _():
            @pl.loop(0, INNER)
            def _(i):
                o_copy(PLANES, part_of, plane, inner, i).wait_recv()

    @pl.loop(0, steps)
    def _(k):
        for_queries(k, lambda copy: copy.wait_send())

    @pl.when(end)
    def _():
        for_queries(PLANES, lambda copy: copy.wait_send())

        @pl.loop(0, INNER)
        def _(i):
            far_query(i).wait_send()

    for_own_weights(lambda copy: copy.wait_send())

    @pl.when(mid)
    def _():
        @pl.loop(pairs - EXTRA_FAR, pairs)
        def _(i):
            w_beyond(1, 1 - piece, i).wait_send()

    @pl.loop(1, steps)
    def _(k):
        @pl.loop(0, pairs)
        def _(i):
            for_forwards(k, i, lambda copy: copy.wait_send())

    @pl.loop(0, PLANES)
    def _(j):
        b = exclusive(plane, j, PLANES) * INNER + inner

        @pl.when(j > 0)
        def _():
            for copy in kv_copies(0, me, b, True):
                copy.wait_send()

        for copy in kv_copies(1, b, across, False):
            copy.wait_send()
        for k in range(2):
            d = exclusive(plane, j, PLANES) * INNER + (inner + 2 * k) % INNER
            for copy in kv_copies(2, d, twin, False):
                copy.wait_send()


def local_any(n, queries, kv_new, kv_cache, kv_gain, w_key, w_value, prefix_len):
    tok = queries.shape[0]
    cac = kv_cache.shape[0]
    heads = w_key.shape[1] // NOPE
    T, C = n * tok, n * cac
    chunks = max(4, n // (2 * INNER))
    hbm = pl.BlockSpec(memory_space=pl.ANY)
    vmem = pl.BlockSpec(memory_space=pltpu.VMEM)
    bf16 = jnp.bfloat16
    dma = pltpu.SemaphoreType.DMA
    return pl.pallas_call(
        functools.partial(kernel, n, tok, cac, heads, chunks),
        out_shape=jax.ShapeDtypeStruct((tok, n * heads * VH), bf16),
        in_specs=[hbm] * 5 + [vmem] * 2 + [pl.BlockSpec(memory_space=pltpu.SMEM)],
        out_specs=hbm,
        scratch_shapes=[
            pltpu.VMEM((2, T // 2, heads * WIDTH), bf16),
            pltpu.VMEM((T, LATENT + ROPE), bf16),
            pltpu.VMEM((C, LATENT + ROPE), bf16),
            pltpu.VMEM((2, 2, LATENT, heads * NOPE), bf16),
            pltpu.VMEM((heads, C + T, 256), bf16),
            pltpu.VMEM((C + T, heads * VH), bf16),
            pltpu.VMEM((INNER * tok, C + T), jnp.float32),
            pltpu.VMEM((2, T // 2, heads * VH), bf16),
            pltpu.VMEM((T, 128), jnp.float32),
            pltpu.VMEM((T, 128), jnp.float32),
            dma((6,)),
            dma((2,)),
            dma((2, n)),
            dma((2, n)),
            dma((6, n)),
            dma((2, n)),
            dma((2, n)),
            dma((2, n)),
            dma((2, chunks)),
            dma((2, chunks)),
        ],
        compiler_params=pltpu.CompilerParams(
            collective_id=0, has_side_effects=True, vmem_limit_bytes=60 * 2**20
        ),
        name="latent_attention",
    )(queries, kv_new, kv_cache, w_key, w_value, kv_gain[None, :], inverse_lanes(), prefix_len)


def local_planes(n, queries, kv_new, kv_cache, kv_gain, w_key, w_value, prefix_len):
    tok = queries.shape[0]
    cac = kv_cache.shape[0]
    heads = w_key.shape[1] // NOPE
    T, C = n * tok, n * cac
    S = T + C
    rows = INNER * tok
    pairs = heads // 2
    hbm = pl.BlockSpec(memory_space=pl.ANY)
    vmem = pl.BlockSpec(memory_space=pltpu.VMEM)
    bf16, f32 = jnp.bfloat16, jnp.float32
    dma = pltpu.SemaphoreType.DMA
    return pl.pallas_call(
        functools.partial(planes_kernel, n, tok, cac, heads),
        out_shape=jax.ShapeDtypeStruct((tok, n * heads * VH), bf16),
        in_specs=[hbm] * 5 + [vmem] * 2 + [pl.BlockSpec(memory_space=pltpu.SMEM)],
        out_specs=hbm,
        scratch_shapes=[
            pltpu.VMEM((PLANES + 1, rows, heads * WIDTH), bf16),
            pltpu.VMEM((T, LATENT + ROPE), bf16),
            pltpu.VMEM((C, LATENT + ROPE), bf16),
            pltpu.VMEM((PLANES, 2, pairs, LATENT, 2 * NOPE), bf16),
            pltpu.VMEM((S, LATENT), bf16),
            pltpu.VMEM((S, 128), f32),
            pltpu.VMEM((heads, S, 256), bf16),
            pltpu.VMEM((heads, S, 256), bf16),
            pltpu.VMEM((rows, rows), f32),
            pltpu.VMEM((rows, S), f32),
            pltpu.VMEM((rows, S), f32),
            pltpu.VMEM((rows, S), bf16),
            pltpu.VMEM((rows, S), bf16),
            pltpu.VMEM((PLANES + 1, rows, heads * VH), bf16),
            pltpu.VMEM((T, 128), f32),
            pltpu.VMEM((T, 128), f32),
            dma((3,)),
            dma((2, pairs)),
            dma((PLANES,)),
            dma((PLANES, 2)),
            dma((PLANES + 2, INNER)),
            dma((PLANES + 1, INNER)),
            dma((6, n)),
            dma((2, n)),
            dma((PLANES + 1, 2, INNER)),
            dma((PLANES + 1, 2, INNER)),
            dma((3, PLANES, 2, pairs)),
            dma((PLANES, 2, pairs)),
        ],
        compiler_params=pltpu.CompilerParams(
            collective_id=0, has_side_effects=True, vmem_limit_bytes=60 * 2**20
        ),
        name="latent_attention",
    )(queries, kv_new, kv_cache, w_key, w_value, kv_gain[None, :], inverse_lanes(), prefix_len)


def local(n, *operands):
    run = local_planes if n == PLANES * INNER else local_any
    return run(n, *operands)


def solution(mesh):
    placed = (
        P(("groups", "seq"), None),
        P(("groups", "seq"), None),
        P(("groups", "seq"), None),
        P(),
        P(None, "seq"),
        P(None, "seq"),
        P("groups"),
    )
    return jax.shard_map(
        functools.partial(local, mesh.shape["seq"]),
        mesh=mesh,
        in_specs=placed,
        out_specs=P(("groups", "seq"), None),
        check_vma=False,
    )
```

```python
import functools
import math

import jax
import jax.numpy as jnp
from jax import lax
from jax.experimental import pallas as pl
from jax.experimental.pallas import tpu as pltpu
from jax.sharding import PartitionSpec as P

NOPE = 128
ROPE = 64
LATENT = 512
VH = 128
WIDTH = NOPE + ROPE
INNER = 4

epsilon = 1e-06


def exclusive(a, b, extent):
    result = 0
    bit = 1
    while bit < extent:
        result = result + ((a // bit + b // bit) % 2) * bit
        bit *= 2
    return result


def inverse_lanes():
    half = ROPE // 2
    inverse = 10000.0 ** (-(jnp.arange(half, dtype=jnp.float32) * 2.0) / ROPE)
    return jnp.concatenate([inverse] * 4)[None, :]


def swap_halves(x, lane):
    return jnp.where(lane % ROPE < ROPE // 2, pltpu.roll(x, 96, 1), pltpu.roll(x, 32, 1))


def kernel(
    n, tok, cac, heads, chunks,
    q_hbm, kvn_hbm, kvc_hbm, wk_hbm, wv_hbm, gain_ref, inverse_ref, plen_ref,
    out_hbm,
    qbuf, kvn, kvc, weights, keys, vals, bias, obuf, cos_ref, sin_ref,
    local_sem, own_out_sem, q_send, q_recv, kv_send, kv_recv, o_send, o_recv, w_send, w_recv,
):
    me = lax.axis_index("seq")
    part = lax.axis_index("groups")
    piece = part % 2
    half = n // 2
    mirror = (me + half) % n
    half_first = (me // half) * half
    half_slabs = half // INNER
    slab = me // INNER
    inner = me % INNER
    slabs = n // INNER
    T, C = n * tok, n * cac
    S = T + C
    qw = heads * WIDTH
    ow = heads * VH
    rows = INNER * tok
    f32, bf16 = jnp.float32, jnp.bfloat16

    def blk(ref, b, size):
        return ref.at[pl.ds(pl.multiple_of(b * size, size), size), :]

    def cols(ref, b, size):
        return ref.at[:, pl.ds(pl.multiple_of(b * size, 128), size)]

    own = [
        pltpu.make_async_copy(kvn_hbm, blk(kvn, me, tok), local_sem.at[0]),
        pltpu.make_async_copy(kvc_hbm, blk(kvc, me, cac), local_sem.at[1]),
        pltpu.make_async_copy(wk_hbm, weights.at[0, 0], local_sem.at[2]),
        pltpu.make_async_copy(wv_hbm, weights.at[1, 0], local_sem.at[3]),
        pltpu.make_async_copy(
            cols(q_hbm, me, qw), blk(qbuf.at[0], me - half_first, tok), local_sem.at[4]
        ),
        pltpu.make_async_copy(
            cols(q_hbm, mirror, qw), blk(qbuf.at[1], me - half_first, tok), local_sem.at[5]
        ),
    ]
    for copy in own:
        copy.start()

    barrier = pltpu.get_barrier_semaphore()

    @pl.loop(1, n)
    def _(i):
        pl.semaphore_signal(barrier, inc=1, device_id={"seq": (me + i) % n})

    beside = {"groups": part + 1 - 2 * piece, "seq": me}
    pl.semaphore_signal(barrier, inc=1, device_id=beside)
    pl.semaphore_wait(barrier, n)

    def kv_copies(stage, b, peer, from_hbm):
        slot = b if stage else peer
        return [
            pltpu.make_async_remote_copy(
                src_ref=kvn_hbm if from_hbm else blk(kvn, b, tok),
                dst_ref=blk(kvn, b, tok),
                send_sem=kv_send.at[2 * stage, slot],
                recv_sem=kv_recv.at[0, b],
                device_id={"seq": peer},
            ),
            pltpu.make_async_remote_copy(
                src_ref=kvc_hbm if from_hbm else blk(kvc, b, cac),
                dst_ref=blk(kvc, b, cac),
                send_sem=kv_send.at[2 * stage + 1, slot],
                recv_sem=kv_recv.at[1, b],
                device_id={"seq": peer},
            ),
        ]

    def q_copy(k, peer, source):
        return pltpu.make_async_remote_copy(
            src_ref=cols(q_hbm, (peer + k * half) % n, qw),
            dst_ref=blk(qbuf.at[k], source - half_first, tok),
            send_sem=q_send.at[k, peer],
            recv_sem=q_recv.at[k, source],
            device_id={"seq": peer},
        )

    def o_copy(k, peer, source):
        return pltpu.make_async_remote_copy(
            src_ref=blk(obuf.at[k], peer - half_first, tok),
            dst_ref=cols(out_hbm, (source + k * half) % n, ow),
            send_sem=o_send.at[k, peer],
            recv_sem=o_recv.at[k, source],
            device_id={"seq": peer},
        )

    def own_out(k):
        return pltpu.make_async_copy(
            blk(obuf.at[k], me - half_first, tok),
            cols(out_hbm, (me + k * half) % n, ow),
            own_out_sem.at[k],
        )

    deep = LATENT // chunks

    def w_chunk(which, k, i):
        return weights.at[which, k, pl.ds(pl.multiple_of(i * deep, deep), deep), :]

    def w_direct(i):
        return pltpu.make_async_remote_copy(
            src_ref=w_chunk(piece, 0, i),
            dst_ref=w_chunk(piece, 1, i),
            send_sem=w_send.at[0, i],
            recv_sem=w_recv.at[0, i],
            device_id={"seq": mirror},
        )

    def w_beside(which, i):
        return pltpu.make_async_remote_copy(
            src_ref=w_chunk(which, 1, i),
            dst_ref=w_chunk(which, 1, i),
            send_sem=w_send.at[1, i],
            recv_sem=w_recv.at[1, i],
            device_id=beside,
        )

    @pl.loop(1, slabs)
    def _(j):
        for copy in kv_copies(0, me, exclusive(slab, j, slabs) * INNER + inner, True):
            copy.start()

    near = (inner // 2) * 2
    far = (near + 2) % INNER

    def q_near(k):
        @pl.loop(1, half_slabs)
        def _(j):
            other = exclusive(slab, j, slabs) * INNER
            for c in range(2):
                q_copy(k, other + near + c, me).start()

    def q_slab(k):
        @pl.loop(1, INNER)
        def _(i):
            q_copy(k, slab * INNER + (inner + i) % INNER, me).start()

    def q_far(k):
        @pl.loop(1, half_slabs)
        def _(j):
            other = exclusive(slab, j, slabs) * INNER
            for c in range(2):
                q_copy(k, other + far + c, me).start()

    q_near(0)

    across = slab * INNER + (inner + 2) % INNER
    twin = me + 1 - 2 * (me % 2)
    own[0].wait()
    own[1].wait()

    @pl.loop(0, slabs)
    def _(j):
        b = exclusive(slab, j, slabs) * INNER + inner

        @pl.when(j > 0)
        def _():
            for copy in kv_copies(0, b, twin, False):
                copy.wait_recv()

        for copy in kv_copies(1, b, across, False):
            copy.start()
        for copy in kv_copies(2, b, twin, False):
            copy.start()

    q_slab(0)

    @pl.loop(0, slabs)
    def _(j):
        b = exclusive(slab, j, slabs) * INNER + (inner + 2) % INNER
        for copy in kv_copies(1, b, twin, False):
            copy.wait_recv()
        for copy in kv_copies(2, b, twin, False):
            copy.start()

    q_far(0)
    own[2].wait()
    own[3].wait()

    @pl.loop(0, chunks)
    def _(i):
        w_direct(i).start()

    q_near(1)
    q_slab(1)
    q_far(1)

    csize = math.gcd(C, 256)
    tsize = math.gcd(T, 256)

    @pl.loop(0, T // tsize)
    def _(i):
        first = pl.multiple_of(i * tsize, tsize)
        at = pl.ds(first, tsize)
        lane = lax.broadcasted_iota(jnp.int32, (tsize, 128), 1)
        position = plen_ref[0] + first + lax.broadcasted_iota(jnp.int32, (tsize, 128), 0)
        phase = position.astype(f32) * inverse_ref[...]
        cos_ref[at, :] = jnp.cos(phase)
        sine = jnp.sin(phase)
        sin_ref[at, :] = jnp.where(lane % ROPE < ROPE // 2, -sine, sine)

    @pl.loop(0, slabs)
    def _(j):
        for k in range(2):
            b = exclusive(slab, j, slabs) * INNER + (twin + 2 * k) % INNER
            for copy in kv_copies(2, b, twin, False):
                copy.wait_recv()

    own[4].wait()
    own[5].wait()

    def project(k, latent, rope, first, size):
        lane = lax.broadcasted_iota(jnp.int32, (size, 128), 1)
        at = pl.ds(first, size)
        rope_even = jnp.where(lane < ROPE, rope, 0.0).astype(bf16)
        for h in range(0, heads, 2):
            pair = jnp.dot(latent, weights[0, k, :, h * NOPE : (h + 2) * NOPE], preferred_element_type=f32)
            keys[h, at, 0:128] = pair[:, :128].astype(bf16)
            keys[h, at, 128:256] = rope_even
            turned = pltpu.roll(pair[:, 128:], 64, 1)
            keys[h + 1, at, 0:128] = jnp.where(lane < ROPE, 0.0, turned).astype(bf16)
            keys[h + 1, at, 128:256] = jnp.where(lane < ROPE, turned, rope).astype(bf16)
            vals[at, h * VH : (h + 2) * VH] = jnp.dot(
                latent, weights[1, k, :, h * VH : (h + 2) * VH], preferred_element_type=f32
            ).astype(bf16)

    scale = math.log2(math.e) / math.sqrt(WIDTH)
    per_slab = chunks // half_slabs

    @pl.loop(0, 2)
    def _(k):
        @pl.when(k == 1)
        def _():
            @pl.loop(0, chunks)
            def _(i):
                w_beside(1 - piece, i).wait_recv()

        @pl.loop(0, C // csize)
        def _(i):
            first = pl.multiple_of(i * csize, csize)
            raw = kvc[pl.ds(first, csize), :]
            rope = raw[:, LATENT:].astype(f32)
            project(k, raw[:, :LATENT], jnp.concatenate([rope, rope], 1), first, csize)

        @pl.loop(0, T // tsize)
        def _(i):
            first = pl.multiple_of(i * tsize, tsize)
            at = pl.ds(first, tsize)
            raw = kvn[at, :]
            wide = raw[:, :LATENT].astype(f32)
            inv = lax.rsqrt(jnp.mean(wide * wide, axis=1, keepdims=True) + epsilon)
            latent = (wide * inv * gain_ref[...]).astype(bf16)
            rope = raw[:, LATENT:].astype(f32)
            rope = jnp.concatenate([rope, rope], 1)
            lane = lax.broadcasted_iota(jnp.int32, (tsize, 128), 1)
            rope = rope * cos_ref[at, :] + swap_halves(rope, lane) * sin_ref[at, :]
            project(k, latent, rope, pl.multiple_of(C + first, tsize), tsize)

        @pl.loop(0, half_slabs)
        def _(j):
            group = exclusive(slab, j + k * (half_slabs - 1 - 2 * j), slabs)

            @pl.loop(0, INNER)
            def _(i):
                b = group * INNER + i

                @pl.when(b != me)
                def _():
                    q_copy(k, me, b).wait_recv()

            base = pl.multiple_of(group * rows, rows)
            at = pl.ds(base, rows)
            near_at = pl.ds(pl.multiple_of(base - half_first * tok, rows), rows)
            row = base + lax.broadcasted_iota(jnp.int32, (rows, S), 0)
            col = lax.broadcasted_iota(jnp.int32, (rows, S), 1)
            live = ((col < C) & (col < plen_ref[0])) | ((col >= C) & (col - C <= row))
            bias[...] = jnp.where(live, 0.0, -1e30)

            @pl.loop(0, heads // 2)
            def _(p):
                lane = lax.broadcasted_iota(jnp.int32, (rows, 128), 1)
                cosine = cos_ref[at, :]
                sine = sin_ref[at, :]

                def third(i):
                    return qbuf[k, near_at, pl.ds(pl.multiple_of(p * 384 + 128 * i, 128), 128)]

                def turn(x, hit):
                    x = x.astype(f32)
                    y = x * cosine + swap_halves(x, lane) * sine
                    return jnp.where(hit, y, x).astype(bf16)

                front = third(0)
                middle = turn(third(1), lane < ROPE)
                back = turn(third(2), lane >= ROPE)
                for side, query in enumerate(
                    (jnp.concatenate([front, middle], 1), jnp.concatenate([middle, back], 1))
                ):
                    h = 2 * p + side
                    scores = lax.dot_general(
                        query, keys[h], (((1,), (1,)), ((), ())), preferred_element_type=f32
                    )
                    scores = scores * scale + bias[...]
                    top = jnp.max(scores, axis=1, keepdims=True)
                    grown = jnp.exp2(scores - top)
                    total = jnp.sum(grown, axis=1, keepdims=True)
                    across_v = pl.ds(pl.multiple_of(h * VH, VH), VH)
                    mixed = jnp.dot(grown.astype(bf16), vals[:, across_v], preferred_element_type=f32)
                    obuf[k, near_at, across_v] = (mixed / total).astype(bf16)

            @pl.loop(0, INNER)
            def _(i):
                b = group * INNER + i

                @pl.when(b != me)
                def _():
                    o_copy(k, b, me).start()

                @pl.when(b == me)
                def _():
                    own_out(k).start()

            @pl.when(k == 0)
            def _():
                @pl.loop(j * per_slab, (j + 1) * per_slab)
                def _(i):
                    w_direct(i).wait_recv()
                    w_beside(piece, i).start()

    for k in range(2):
        own_out(k).wait()

        @pl.loop(1, half)
        def _(i):
            peer = half_first + (me + i) % half
            q_copy(k, peer, me).wait_send()
            o_copy(k, peer, me).wait_send()
            o_copy(k, me, peer).wait_recv()

    @pl.loop(0, chunks)
    def _(i):
        w_direct(i).wait_send()
        w_beside(piece, i).wait_send()

    @pl.loop(0, slabs)
    def _(j):
        b = exclusive(slab, j, slabs) * INNER + inner

        @pl.when(j > 0)
        def _():
            for copy in kv_copies(0, me, b, True):
                copy.wait_send()

        for copy in kv_copies(1, b, across, False):
            copy.wait_send()
        for k in range(2):
            d = exclusive(slab, j, slabs) * INNER + (inner + 2 * k) % INNER
            for copy in kv_copies(2, d, twin, False):
                copy.wait_send()


PLANES = 4
EXTRA_END = 3
EXTRA_MIDDLE = 0
EXTRA_FAR = 1


def planes_kernel(
    n, tok, cac, heads,
    q_hbm, kvn_hbm, kvc_hbm, wk_hbm, wv_hbm, gain_ref, inverse_ref, plen_ref,
    out_hbm,
    qbuf, kvn, kvc, weights, latents, aux, keys, vals, bias, score_a, score_b, prob_a, prob_b, obuf,
    cos_ref, sin_ref,
    local_sem, own_w_sem, own_q_sem, own_out_sem, q_send, q_recv, kv_send, kv_recv, o_send, o_recv, w_send, w_recv,
):
    me = lax.axis_index("seq")
    part = lax.axis_index("groups")
    piece = part % 2
    plane = me // INNER
    inner = me % INNER
    side = plane // (PLANES // 2)
    last = PLANES - 1

    def whole(r):
        return r + side * (last - 2 * r)

    middle = whole(plane)
    end = middle == 0
    mid = middle == 1
    T, C = n * tok, n * cac
    S = T + C
    qw = heads * WIDTH
    ow = heads * VH
    rows = INNER * tok
    pairs = heads // 2
    f32, bf16 = jnp.float32, jnp.bfloat16
    scale = math.log2(math.e) / math.sqrt(WIDTH)

    def blk(ref, b, size):
        return ref.at[pl.ds(pl.multiple_of(b * size, size), size), :]

    def cols(ref, b, size):
        return ref.at[:, pl.ds(pl.multiple_of(b * size, 128), size)]

    def head_plane(k):
        return whole(jnp.where(end, k, jnp.where(k == 0, 1, jnp.where(k == 1, 0, k))))

    steps = 3 + middle

    def own_q(k):
        return pltpu.make_async_copy(
            cols(q_hbm, head_plane(k) * INNER + inner, qw), blk(qbuf.at[k], inner, tok), own_q_sem.at[k]
        )

    own = [
        pltpu.make_async_copy(kvn_hbm, blk(kvn, me, tok), local_sem.at[0]),
        pltpu.make_async_copy(kvc_hbm, blk(kvc, me, cac), local_sem.at[1]),
    ]
    for copy in own:
        copy.start()

    def own_w(which, i):
        source = wv_hbm if which else wk_hbm
        return pltpu.make_async_copy(cols(source, i, 2 * NOPE), weights.at[0, which, i], own_w_sem.at[which, i])

    for which in range(2):
        @pl.loop(0, pairs)
        def _(i):
            own_w(which, i).start()

    barrier = pltpu.get_barrier_semaphore()

    @pl.loop(1, n)
    def _(i):
        pl.semaphore_signal(barrier, inc=1, device_id={"seq": (me + i) % n})

    beside = {"groups": part + 1 - 2 * piece, "seq": me}
    pl.semaphore_signal(barrier, inc=1, device_id=beside)
    pl.semaphore_wait(barrier, n)

    def kv_copies(stage, b, peer, from_hbm):
        slot = b if stage else peer
        return [
            pltpu.make_async_remote_copy(
                src_ref=kvn_hbm if from_hbm else blk(kvn, b, tok),
                dst_ref=blk(kvn, b, tok),
                send_sem=kv_send.at[2 * stage, slot],
                recv_sem=kv_recv.at[0, b],
                device_id={"seq": peer},
            ),
            pltpu.make_async_remote_copy(
                src_ref=kvc_hbm if from_hbm else blk(kvc, b, cac),
                dst_ref=blk(kvc, b, cac),
                send_sem=kv_send.at[2 * stage + 1, slot],
                recv_sem=kv_recv.at[1, b],
                device_id={"seq": peer},
            ),
        ]

    near = {"seq": whole(1 - middle) * INNER + inner}
    beyond = {"seq": whole(2) * INNER + inner}

    def far_query(source):
        return pltpu.make_async_remote_copy(
            src_ref=blk(qbuf.at[PLANES], source, tok),
            dst_ref=blk(qbuf.at[PLANES], source, tok),
            send_sem=q_send.at[PLANES + 1, source],
            recv_sem=q_recv.at[PLANES, source],
            device_id=near,
        )

    def q_copy(k, to_plane, to, source):
        columns = jnp.where(k == PLANES, whole(last), head_plane(k)) * INNER + to
        return pltpu.make_async_remote_copy(
            src_ref=cols(q_hbm, columns, qw),
            dst_ref=blk(qbuf.at[k], source, tok),
            send_sem=q_send.at[k, to],
            recv_sem=q_recv.at[k, source],
            device_id={"seq": to_plane * INNER + to},
        )

    def o_part(k, part_of, to):
        return obuf.at[k, pl.ds(pl.multiple_of(to * tok, tok), tok), pl.ds(pl.multiple_of(part_of * ow // 2, 128), ow // 2)]

    def o_copy(k, part_of, to_plane, to, source):
        columns = jnp.where(k == PLANES, whole(last), head_plane(k)) * INNER + source
        return pltpu.make_async_remote_copy(
            src_ref=o_part(k, part_of, to),
            dst_ref=cols(out_hbm, 2 * columns + part_of, ow // 2),
            send_sem=o_send.at[k, part_of, to],
            recv_sem=o_recv.at[k, part_of, source],
            device_id={"seq": to_plane * INNER + to},
        )

    def own_out(k, part_of):
        columns = head_plane(k) * INNER + inner
        return pltpu.make_async_copy(
            o_part(k, part_of, inner), cols(out_hbm, 2 * columns + part_of, ow // 2), own_out_sem.at[k, part_of]
        )

    def w_chunk(k, which, i):
        return weights.at[k, which, i]

    def w_copy(way, k, to_k, which, i, device):
        return pltpu.make_async_remote_copy(
            src_ref=w_chunk(k, which, i),
            dst_ref=w_chunk(to_k, which, i),
            send_sem=w_send.at[way, k, which, i],
            recv_sem=w_recv.at[to_k, which, i],
            device_id=device,
        )

    def w_near(k, which, i):
        return w_copy(0, k, jnp.where(k == 0, 1, 2), which, i, near)

    def w_beyond(k, which, i):
        return w_copy(1, k, k + 2, which, i, beyond)

    def w_beside(k, i):
        return w_copy(2, k, k, piece, i, beside)

    def extras(k):
        return jnp.where(mid, jnp.where(k == 1, EXTRA_END, jnp.where(k == 2, EXTRA_MIDDLE, EXTRA_FAR)), 0)

    late_pair = pairs - 2

    def for_own_weights(do):
        @pl.loop(0, pairs)
        def _(i):
            do(w_near(0, piece, i))

            @pl.when(mid)
            def _():
                do(w_beyond(0, piece, i))

        @pl.when(end)
        def _():
            @pl.loop(pairs - EXTRA_END, pairs)
            def _(i):
                @pl.when(i != late_pair)
                def _():
                    do(w_near(0, 1 - piece, i))

        @pl.when(mid)
        def _():
            @pl.loop(pairs - EXTRA_MIDDLE, pairs)
            def _(i):
                do(w_beyond(0, 1 - piece, i))

    def for_forwards(k, i, do):
        @pl.when(mid & (k == 1))
        def _():
            do(w_beyond(k, piece, i))

        @pl.when(mid & (k == 2))
        def _():
            do(w_near(k, piece, i))

        @pl.when(i < pairs - extras(k))
        def _():
            do(w_beside(k, i))

    def pass_on(k, i):
        w_copy(2, k, k, piece, i, beside).wait_recv()
        for_forwards(k, i, lambda copy: copy.start())

    @pl.loop(1, PLANES)
    def _(j):
        for copy in kv_copies(0, me, exclusive(plane, j, PLANES) * INNER + inner, True):
            copy.start()

    for which in range(2):
        @pl.loop(0, pairs)
        def _(i):
            own_w(which, i).wait()

    for_own_weights(lambda copy: copy.start())

    across = plane * INNER + (inner + 2) % INNER
    twin = me + 1 - 2 * (me % 2)
    own[0].wait()
    own[1].wait()

    own_far_q = pltpu.make_async_copy(
        cols(q_hbm, whole(last) * INNER + inner, qw), blk(qbuf.at[PLANES], inner, tok), local_sem.at[2]
    )

    @pl.when(end)
    def _():
        own_far_q.start()

    @pl.loop(0, steps)
    def _(k):
        own_q(k).start()

    def for_queries(k, do):
        @pl.loop(1, INNER)
        def _(i):
            do(q_copy(k, plane, (inner + i) % INNER, inner))

    def relay_kv(p):
        b = p * INNER + inner
        for copy in kv_copies(1, b, across, False):
            copy.start()
        for copy in kv_copies(2, b, twin, False):
            copy.start()

    relay_kv(plane)
    for_queries(0, lambda copy: copy.start())

    @pl.loop(1, PLANES)
    def _(j):
        p = exclusive(plane, j, PLANES)
        for copy in kv_copies(0, p * INNER + inner, twin, False):
            copy.wait_recv()
        relay_kv(p)

    @pl.when(end)
    def _():
        for_queries(PLANES, lambda copy: copy.start())
        for_queries(1, lambda copy: copy.start())
        for_queries(2, lambda copy: copy.start())

    @pl.when(mid)
    def _():
        for k in (2, 1, 3):
            for_queries(k, lambda copy: copy.start())

    tsize = math.gcd(T, 256)
    csize = math.gcd(C, 256)

    @pl.loop(0, T // tsize)
    def _(i):
        first = pl.multiple_of(i * tsize, tsize)
        at = pl.ds(first, tsize)
        lane = lax.broadcasted_iota(jnp.int32, (tsize, 128), 1)
        position = plen_ref[0] + first + lax.broadcasted_iota(jnp.int32, (tsize, 128), 0)
        phase = position.astype(f32) * inverse_ref[...]
        cos_ref[at, :] = jnp.cos(phase)
        sine = jnp.sin(phase)
        sin_ref[at, :] = jnp.where(lane % ROPE < ROPE // 2, -sine, sine)

    bias[...] = jnp.where(
        lax.broadcasted_iota(jnp.int32, (rows, rows), 1) <= lax.broadcasted_iota(jnp.int32, (rows, rows), 0),
        0.0, -1e30,
    )

    def pass_on_near(i):
        pass_on(1, i)

        @pl.when(mid)
        def _():
            pass_on(2, i)

    pass_on_near(0)

    @pl.loop(0, PLANES)
    def _(j):
        b = exclusive(plane, j, PLANES) * INNER + (inner + 2) % INNER
        for copy in kv_copies(1, b, twin, False):
            copy.wait_recv()
        for copy in kv_copies(2, b, twin, False):
            copy.start()

    pass_on_near(1)

    @pl.loop(0, heads)
    def _(h):
        vals[h, :, 128:256] = jnp.ones((S, 128), bf16)

    @pl.loop(0, PLANES)
    def _(j):
        for k in range(2):
            b = exclusive(plane, j, PLANES) * INNER + (twin + 2 * k) % INNER
            for copy in kv_copies(2, b, twin, False):
                copy.wait_recv()

    def keep_rope(first, size, rope, dead):
        at = pl.ds(first, size)
        lane = lax.broadcasted_iota(jnp.int32, (size, 128), 1)
        low = lane < ROPE
        aux[at, :] = jnp.where(low, jnp.where(lane == 0, dead, 0.0), rope)
        tail = jnp.where(low, rope, jnp.where(lane == ROPE, dead, 0.0)).astype(bf16)
        for h in range(0, heads, 2):
            keys[h, at, 128:256] = tail

    @pl.loop(0, C // csize)
    def _(i):
        first = pl.multiple_of(i * csize, csize)
        raw = kvc[pl.ds(first, csize), :]
        latents[pl.ds(first, csize), :] = raw[:, :LATENT]
        rope = raw[:, LATENT:].astype(f32)
        row = first + lax.broadcasted_iota(jnp.int32, (csize, 128), 0)
        dead = jnp.where(row < plen_ref[0], 0.0, -1e30)
        keep_rope(first, csize, jnp.concatenate([rope, rope], 1), dead)

    @pl.loop(0, T // tsize)
    def _(i):
        first = pl.multiple_of(i * tsize, tsize)
        at = pl.ds(first, tsize)
        raw = kvn[at, :]
        wide = raw[:, :LATENT].astype(f32)
        inv = lax.rsqrt(jnp.mean(wide * wide, axis=1, keepdims=True) + epsilon)
        latents[pl.ds(pl.multiple_of(C + first, tsize), tsize), :] = (wide * inv * gain_ref[...]).astype(bf16)
        rope = raw[:, LATENT:].astype(f32)
        rope = jnp.concatenate([rope, rope], 1)
        lane = lax.broadcasted_iota(jnp.int32, (tsize, 128), 1)
        rope = rope * cos_ref[at, :] + swap_halves(rope, lane) * sin_ref[at, :]
        keep_rope(pl.multiple_of(C + first, tsize), tsize, rope, 0.0)
        cos_ref[at, :] = cos_ref[at, :] * scale
        sin_ref[at, :] = sin_ref[at, :] * scale

    pass_on_near(2)
    size = math.gcd(C, rows)

    def project_rows(k, p, live):
        lane = lax.broadcasted_iota(jnp.int32, (size, 128), 1)
        for first in range(0, live, size):
            at = slice(first, first + size)
            latent = latents[at, :]
            rest = aux[at, :]
            pair = jnp.dot(latent, weights[k, 0, p], preferred_element_type=f32) * scale
            keys[2 * p, at, 0:128] = pair[:, :128].astype(bf16)
            turned = pltpu.roll(pair[:, 128:], 64, 1)
            keys[2 * p + 1, at, 0:128] = jnp.where(lane < ROPE, rest, turned).astype(bf16)
            keys[2 * p + 1, at, 128:256] = jnp.where(lane < ROPE, turned, rest).astype(bf16)
            both = jnp.dot(latent, weights[k, 1, p], preferred_element_type=f32).astype(bf16)
            vals[2 * p, at, 0:128] = both[:, :128]
            vals[2 * p + 1, at, 0:128] = both[:, 128:]

    def project(k, p):
        top_plane = jnp.where(mid & (k == last), jnp.maximum(plane, whole(0)), plane)
        for s in range(PLANES):
            @pl.when(top_plane == s)
            def _():
                project_rows(k, p, C + (s + 1) * rows)

    def attend(slot, first_row, live, first_pair, last_pair):
        cut = live - rows

        def rotated(p):
            at = pl.ds(first_row, rows)
            lane = lax.broadcasted_iota(jnp.int32, (rows, 128), 1)
            cosine = cos_ref[at, :]
            sine = sin_ref[at, :]

            def third(i):
                return qbuf[slot, :, pl.ds(pl.multiple_of(p * 3 * 128 + 128 * i, 128), 128)]

            def turn(x, hit):
                x = x.astype(f32)
                y = x * cosine + swap_halves(x, lane) * sine
                return jnp.where(hit, y, x)

            centre = turn(third(1), lane < ROPE)
            return (
                jnp.concatenate([third(0), jnp.where(lane == ROPE, 1.0, centre).astype(bf16)], 1),
                jnp.concatenate(
                    [jnp.where(lane == 0, 1.0, centre).astype(bf16), turn(third(2), lane >= ROPE).astype(bf16)], 1
                ),
            )

        def score(query, h, into):
            into[:, 0:live] = lax.dot_general(
                query, keys[h, 0:live, :], (((1,), (1,)), ((), ())), preferred_element_type=f32
            )

        def soften(scores, into):
            for r in range(0, rows, 16):
                before = scores[r : r + 16, 0:cut]
                near_end = scores[r : r + 16, cut:live] + bias[r : r + 16, :]
                top = jnp.maximum(
                    jnp.max(before, axis=1, keepdims=True), jnp.max(near_end, axis=1, keepdims=True)
                )
                into[r : r + 16, 0:cut] = jnp.exp2(before - top).astype(bf16)
                into[r : r + 16, cut:live] = jnp.exp2(near_end - top).astype(bf16)

        def mix(probs, h):
            mixed = jnp.dot(probs[:, 0:live], vals[h, 0:live, :], preferred_element_type=f32)
            obuf[slot, :, pl.ds(pl.multiple_of(h * VH, VH), VH)] = (mixed[:, :VH] / mixed[:, VH:]).astype(bf16)

        @pl.loop(first_pair, last_pair)
        def _(p):
            done = jnp.maximum(p - 1, first_pair)
            even, odd = rotated(p)
            score(even, 2 * p, score_a)
            soften(score_b, prob_b)
            mix(prob_a, 2 * done)
            soften(score_a, prob_a)
            mix(prob_b, 2 * done + 1)
            score(odd, 2 * p + 1, score_b)

        soften(score_b, prob_b)
        mix(prob_a, 2 * last_pair - 2)
        mix(prob_b, 2 * last_pair - 1)

    def attend_plane(slot, s, first_pair, last_pair):
        for plane_of in range(PLANES):
            @pl.when(s == plane_of)
            def _():
                attend(slot, plane_of * rows, C + (plane_of + 1) * rows, first_pair, last_pair)

    def other_kind(k, p):
        return w_copy(2, k, k, 1 - piece, p, beside)

    @pl.loop(0, jnp.where(end, 5, 7))
    def _(turn):
        ends_k = 1 + (turn - 1) // 2
        mids_k = jnp.where(turn <= 2, 2, jnp.where((turn == 3) | (turn == 6), 1, last))
        k = jnp.where(turn == 0, 0, jnp.where(end, ends_k, mids_k))
        ends_half = (turn + 1) % 2
        mids_half = jnp.where((turn == 2) | (turn >= 5), 1, 0)
        half = jnp.where(turn == 0, 0, jnp.where(end, ends_half, mids_half))
        far = mid & (k == last)
        first_pair = half * (pairs // 2)
        last_pair = jnp.where(turn == 0, pairs, first_pair + pairs // 2)

        @pl.when(mid & (turn == 5))
        def _():
            pass_on(3, 3)

        @pl.loop(first_pair, last_pair)
        def _(p):
            @pl.when((k > 0) & ~(mid & (k == 1) & (p >= pairs - EXTRA_FAR)))
            def _():
                other_kind(k, p).wait_recv()

            project(k, p)

        @pl.when(half == 0)
        def _():
            own_q(k).wait()

            @pl.loop(1, INNER)
            def _(i):
                q_copy(k, plane, inner, (inner + i) % INNER).wait_recv()

        @pl.when(turn == 0)
        def _():
            pass_on_near(3)

        @pl.when(end & (turn == 3))
        def _():
            pass_on(2, 2)

        @pl.loop(jnp.where(far, 0, 1), 2)
        def _(item):
            far_item = far & (item == jnp.where(turn == 5, 0, 1))

            @pl.when(far_item & (turn == 4))
            def _():
                @pl.loop(0, INNER)
                def _(i):
                    far_query(i).wait_recv()

            slot = jnp.where(far_item, PLANES, k)
            attend_plane(slot, jnp.where(far_item, whole(0), plane), first_pair, last_pair)

            @pl.loop(first_pair // (pairs // 2), last_pair // (pairs // 2))
            def _(part_of):
                @pl.when(far_item)
                def _():
                    @pl.loop(0, INNER)
                    def _(i):
                        o_copy(PLANES, part_of, whole(0), (inner + i) % INNER, inner).start()

                @pl.when(~far_item)
                def _():
                    own_out(k, part_of).start()

                    @pl.loop(1, INNER)
                    def _(i):
                        o_copy(k, part_of, plane, (inner + i) % INNER, inner).start()

        @pl.when(end & (turn > 0) & (turn < 4))
        def _():
            pass_on(2, jnp.where(turn == 3, 3, turn - 1))

        @pl.when(mid & ((turn < 2) | (turn == 3)))
        def _():
            pass_on(3, jnp.where(turn == 3, 2, turn))

        @pl.when(mid & (turn == 1))
        def _():
            @pl.loop(pairs - EXTRA_FAR, pairs)
            def _(p):
                other_kind(1, p).wait_recv()
                w_beyond(1, 1 - piece, p).start()

        @pl.when(end & (turn == 0))
        def _():
            @pl.loop(1, INNER)
            def _(i):
                q_copy(PLANES, plane, inner, (inner + i) % INNER).wait_recv()

            own_far_q.wait()

            @pl.loop(0, INNER)
            def _(i):
                far_query(i).start()

            w_near(0, 1 - piece, late_pair).start()

    @pl.loop(0, 2)
    def _(part_of):
        @pl.loop(0, steps)
        def _(k):
            own_out(k, part_of).wait()

            @pl.loop(1, INNER)
            def _(i):
                o_copy(k, part_of, plane, (inner + i) % INNER, inner).wait_send()
                o_copy(k, part_of, plane, inner, (inner + i) % INNER).wait_recv()

        @pl.when(mid)
        def _():
            @pl.loop(0, INNER)
            def _(i):
                o_copy(PLANES, part_of, whole(0), (inner + i) % INNER, inner).wait_send()

        @pl.when(end)
        def _():
            @pl.loop(0, INNER)
            def _(i):
                o_copy(PLANES, part_of, plane, inner, i).wait_recv()

    @pl.loop(0, steps)
    def _(k):
        for_queries(k, lambda copy: copy.wait_send())

    @pl.when(end)
    def _():
        for_queries(PLANES, lambda copy: copy.wait_send())

        @pl.loop(0, INNER)
        def _(i):
            far_query(i).wait_send()

        w_near(0, 1 - piece, late_pair).wait_send()

    for_own_weights(lambda copy: copy.wait_send())

    @pl.when(mid)
    def _():
        @pl.loop(pairs - EXTRA_FAR, pairs)
        def _(i):
            w_beyond(1, 1 - piece, i).wait_send()

    @pl.loop(1, steps)
    def _(k):
        @pl.loop(0, pairs)
        def _(i):
            for_forwards(k, i, lambda copy: copy.wait_send())

    @pl.loop(0, PLANES)
    def _(j):
        b = exclusive(plane, j, PLANES) * INNER + inner

        @pl.when(j > 0)
        def _():
            for copy in kv_copies(0, me, b, True):
                copy.wait_send()

        for copy in kv_copies(1, b, across, False):
            copy.wait_send()
        for k in range(2):
            d = exclusive(plane, j, PLANES) * INNER + (inner + 2 * k) % INNER
            for copy in kv_copies(2, d, twin, False):
                copy.wait_send()


def local_any(n, queries, kv_new, kv_cache, kv_gain, w_key, w_value, prefix_len):
    tok = queries.shape[0]
    cac = kv_cache.shape[0]
    heads = w_key.shape[1] // NOPE
    T, C = n * tok, n * cac
    chunks = max(4, n // (2 * INNER))
    hbm = pl.BlockSpec(memory_space=pl.ANY)
    vmem = pl.BlockSpec(memory_space=pltpu.VMEM)
    bf16 = jnp.bfloat16
    dma = pltpu.SemaphoreType.DMA
    return pl.pallas_call(
        functools.partial(kernel, n, tok, cac, heads, chunks),
        out_shape=jax.ShapeDtypeStruct((tok, n * heads * VH), bf16),
        in_specs=[hbm] * 5 + [vmem] * 2 + [pl.BlockSpec(memory_space=pltpu.SMEM)],
        out_specs=hbm,
        scratch_shapes=[
            pltpu.VMEM((2, T // 2, heads * WIDTH), bf16),
            pltpu.VMEM((T, LATENT + ROPE), bf16),
            pltpu.VMEM((C, LATENT + ROPE), bf16),
            pltpu.VMEM((2, 2, LATENT, heads * NOPE), bf16),
            pltpu.VMEM((heads, C + T, 256), bf16),
            pltpu.VMEM((C + T, heads * VH), bf16),
            pltpu.VMEM((INNER * tok, C + T), jnp.float32),
            pltpu.VMEM((2, T // 2, heads * VH), bf16),
            pltpu.VMEM((T, 128), jnp.float32),
            pltpu.VMEM((T, 128), jnp.float32),
            dma((6,)),
            dma((2,)),
            dma((2, n)),
            dma((2, n)),
            dma((6, n)),
            dma((2, n)),
            dma((2, n)),
            dma((2, n)),
            dma((2, chunks)),
            dma((2, chunks)),
        ],
        compiler_params=pltpu.CompilerParams(
            collective_id=0, has_side_effects=True, vmem_limit_bytes=60 * 2**20
        ),
        name="latent_attention",
    )(queries, kv_new, kv_cache, w_key, w_value, kv_gain[None, :], inverse_lanes(), prefix_len)


def local_planes(n, queries, kv_new, kv_cache, kv_gain, w_key, w_value, prefix_len):
    tok = queries.shape[0]
    cac = kv_cache.shape[0]
    heads = w_key.shape[1] // NOPE
    T, C = n * tok, n * cac
    S = T + C
    rows = INNER * tok
    pairs = heads // 2
    hbm = pl.BlockSpec(memory_space=pl.ANY)
    vmem = pl.BlockSpec(memory_space=pltpu.VMEM)
    bf16, f32 = jnp.bfloat16, jnp.float32
    dma = pltpu.SemaphoreType.DMA
    return pl.pallas_call(
        functools.partial(planes_kernel, n, tok, cac, heads),
        out_shape=jax.ShapeDtypeStruct((tok, n * heads * VH), bf16),
        in_specs=[hbm] * 5 + [vmem] * 2 + [pl.BlockSpec(memory_space=pltpu.SMEM)],
        out_specs=hbm,
        scratch_shapes=[
            pltpu.VMEM((PLANES + 1, rows, heads * WIDTH), bf16),
            pltpu.VMEM((T, LATENT + ROPE), bf16),
            pltpu.VMEM((C, LATENT + ROPE), bf16),
            pltpu.VMEM((PLANES, 2, pairs, LATENT, 2 * NOPE), bf16),
            pltpu.VMEM((S, LATENT), bf16),
            pltpu.VMEM((S, 128), f32),
            pltpu.VMEM((heads, S, 256), bf16),
            pltpu.VMEM((heads, S, 256), bf16),
            pltpu.VMEM((rows, rows), f32),
            pltpu.VMEM((rows, S), f32),
            pltpu.VMEM((rows, S), f32),
            pltpu.VMEM((rows, S), bf16),
            pltpu.VMEM((rows, S), bf16),
            pltpu.VMEM((PLANES + 1, rows, heads * VH), bf16),
            pltpu.VMEM((T, 128), f32),
            pltpu.VMEM((T, 128), f32),
            dma((3,)),
            dma((2, pairs)),
            dma((PLANES,)),
            dma((PLANES, 2)),
            dma((PLANES + 2, INNER)),
            dma((PLANES + 1, INNER)),
            dma((6, n)),
            dma((2, n)),
            dma((PLANES + 1, 2, INNER)),
            dma((PLANES + 1, 2, INNER)),
            dma((3, PLANES, 2, pairs)),
            dma((PLANES, 2, pairs)),
        ],
        compiler_params=pltpu.CompilerParams(
            collective_id=0, has_side_effects=True, vmem_limit_bytes=60 * 2**20
        ),
        name="latent_attention",
    )(queries, kv_new, kv_cache, w_key, w_value, kv_gain[None, :], inverse_lanes(), prefix_len)


def local(n, *operands):
    run = local_planes if n == PLANES * INNER else local_any
    return run(n, *operands)


def solution(mesh):
    placed = (
        P(("groups", "seq"), None),
        P(("groups", "seq"), None),
        P(("groups", "seq"), None),
        P(),
        P(None, "seq"),
        P(None, "seq"),
        P("groups"),
    )
    return jax.shard_map(
        functools.partial(local, mesh.shape["seq"]),
        mesh=mesh,
        in_specs=placed,
        out_specs=P(("groups", "seq"), None),
        check_vma=False,
    )
```

```python
import functools
import math

import jax
import jax.numpy as jnp
from jax import lax
from jax.experimental import pallas as pl
from jax.experimental.pallas import tpu as pltpu
from jax.sharding import PartitionSpec as P

NOPE = 128
ROPE = 64
LATENT = 512
VH = 128
WIDTH = NOPE + ROPE
INNER = 4

epsilon = 1e-06


def exclusive(a, b, extent):
    result = 0
    bit = 1
    while bit < extent:
        result = result + ((a // bit + b // bit) % 2) * bit
        bit *= 2
    return result


def inverse_lanes():
    half = ROPE // 2
    inverse = 10000.0 ** (-(jnp.arange(half, dtype=jnp.float32) * 2.0) / ROPE)
    return jnp.concatenate([inverse] * 4)[None, :]


def swap_halves(x, lane):
    return jnp.where(lane % ROPE < ROPE // 2, pltpu.roll(x, 96, 1), pltpu.roll(x, 32, 1))


def kernel(
    n, tok, cac, heads, chunks,
    q_hbm, kvn_hbm, kvc_hbm, wk_hbm, wv_hbm, gain_ref, inverse_ref, plen_ref,
    out_hbm,
    qbuf, kvn, kvc, weights, keys, vals, bias, obuf, cos_ref, sin_ref,
    local_sem, own_out_sem, q_send, q_recv, kv_send, kv_recv, o_send, o_recv, w_send, w_recv,
):
    me = lax.axis_index("seq")
    part = lax.axis_index("groups")
    piece = part % 2
    half = n // 2
    mirror = (me + half) % n
    half_first = (me // half) * half
    half_slabs = half // INNER
    slab = me // INNER
    inner = me % INNER
    slabs = n // INNER
    T, C = n * tok, n * cac
    S = T + C
    qw = heads * WIDTH
    ow = heads * VH
    rows = INNER * tok
    f32, bf16 = jnp.float32, jnp.bfloat16

    def blk(ref, b, size):
        return ref.at[pl.ds(pl.multiple_of(b * size, size), size), :]

    def cols(ref, b, size):
        return ref.at[:, pl.ds(pl.multiple_of(b * size, 128), size)]

    own = [
        pltpu.make_async_copy(kvn_hbm, blk(kvn, me, tok), local_sem.at[0]),
        pltpu.make_async_copy(kvc_hbm, blk(kvc, me, cac), local_sem.at[1]),
        pltpu.make_async_copy(wk_hbm, weights.at[0, 0], local_sem.at[2]),
        pltpu.make_async_copy(wv_hbm, weights.at[1, 0], local_sem.at[3]),
        pltpu.make_async_copy(
            cols(q_hbm, me, qw), blk(qbuf.at[0], me - half_first, tok), local_sem.at[4]
        ),
        pltpu.make_async_copy(
            cols(q_hbm, mirror, qw), blk(qbuf.at[1], me - half_first, tok), local_sem.at[5]
        ),
    ]
    for copy in own:
        copy.start()

    barrier = pltpu.get_barrier_semaphore()

    @pl.loop(1, n)
    def _(i):
        pl.semaphore_signal(barrier, inc=1, device_id={"seq": (me + i) % n})

    beside = {"groups": part + 1 - 2 * piece, "seq": me}
    pl.semaphore_signal(barrier, inc=1, device_id=beside)
    pl.semaphore_wait(barrier, n)

    def kv_copies(stage, b, peer, from_hbm):
        slot = b if stage else peer
        return [
            pltpu.make_async_remote_copy(
                src_ref=kvn_hbm if from_hbm else blk(kvn, b, tok),
                dst_ref=blk(kvn, b, tok),
                send_sem=kv_send.at[2 * stage, slot],
                recv_sem=kv_recv.at[0, b],
                device_id={"seq": peer},
            ),
            pltpu.make_async_remote_copy(
                src_ref=kvc_hbm if from_hbm else blk(kvc, b, cac),
                dst_ref=blk(kvc, b, cac),
                send_sem=kv_send.at[2 * stage + 1, slot],
                recv_sem=kv_recv.at[1, b],
                device_id={"seq": peer},
            ),
        ]

    def q_copy(k, peer, source):
        return pltpu.make_async_remote_copy(
            src_ref=cols(q_hbm, (peer + k * half) % n, qw),
            dst_ref=blk(qbuf.at[k], source - half_first, tok),
            send_sem=q_send.at[k, peer],
            recv_sem=q_recv.at[k, source],
            device_id={"seq": peer},
        )

    def o_copy(k, peer, source):
        return pltpu.make_async_remote_copy(
            src_ref=blk(obuf.at[k], peer - half_first, tok),
            dst_ref=cols(out_hbm, (source + k * half) % n, ow),
            send_sem=o_send.at[k, peer],
            recv_sem=o_recv.at[k, source],
            device_id={"seq": peer},
        )

    def own_out(k):
        return pltpu.make_async_copy(
            blk(obuf.at[k], me - half_first, tok),
            cols(out_hbm, (me + k * half) % n, ow),
            own_out_sem.at[k],
        )

    deep = LATENT // chunks

    def w_chunk(which, k, i):
        return weights.at[which, k, pl.ds(pl.multiple_of(i * deep, deep), deep), :]

    def w_direct(i):
        return pltpu.make_async_remote_copy(
            src_ref=w_chunk(piece, 0, i),
            dst_ref=w_chunk(piece, 1, i),
            send_sem=w_send.at[0, i],
            recv_sem=w_recv.at[0, i],
            device_id={"seq": mirror},
        )

    def w_beside(which, i):
        return pltpu.make_async_remote_copy(
            src_ref=w_chunk(which, 1, i),
            dst_ref=w_chunk(which, 1, i),
            send_sem=w_send.at[1, i],
            recv_sem=w_recv.at[1, i],
            device_id=beside,
        )

    @pl.loop(1, slabs)
    def _(j):
        for copy in kv_copies(0, me, exclusive(slab, j, slabs) * INNER + inner, True):
            copy.start()

    near = (inner // 2) * 2
    far = (near + 2) % INNER

    def q_near(k):
        @pl.loop(1, half_slabs)
        def _(j):
            other = exclusive(slab, j, slabs) * INNER
            for c in range(2):
                q_copy(k, other + near + c, me).start()

    def q_slab(k):
        @pl.loop(1, INNER)
        def _(i):
            q_copy(k, slab * INNER + (inner + i) % INNER, me).start()

    def q_far(k):
        @pl.loop(1, half_slabs)
        def _(j):
            other = exclusive(slab, j, slabs) * INNER
            for c in range(2):
                q_copy(k, other + far + c, me).start()

    q_near(0)

    across = slab * INNER + (inner + 2) % INNER
    twin = me + 1 - 2 * (me % 2)
    own[0].wait()
    own[1].wait()

    @pl.loop(0, slabs)
    def _(j):
        b = exclusive(slab, j, slabs) * INNER + inner

        @pl.when(j > 0)
        def _():
            for copy in kv_copies(0, b, twin, False):
                copy.wait_recv()

        for copy in kv_copies(1, b, across, False):
            copy.start()
        for copy in kv_copies(2, b, twin, False):
            copy.start()

    q_slab(0)

    @pl.loop(0, slabs)
    def _(j):
        b = exclusive(slab, j, slabs) * INNER + (inner + 2) % INNER
        for copy in kv_copies(1, b, twin, False):
            copy.wait_recv()
        for copy in kv_copies(2, b, twin, False):
            copy.start()

    q_far(0)
    own[2].wait()
    own[3].wait()

    @pl.loop(0, chunks)
    def _(i):
        w_direct(i).start()

    q_near(1)
    q_slab(1)
    q_far(1)

    csize = math.gcd(C, 256)
    tsize = math.gcd(T, 256)

    @pl.loop(0, T // tsize)
    def _(i):
        first = pl.multiple_of(i * tsize, tsize)
        at = pl.ds(first, tsize)
        lane = lax.broadcasted_iota(jnp.int32, (tsize, 128), 1)
        position = plen_ref[0] + first + lax.broadcasted_iota(jnp.int32, (tsize, 128), 0)
        phase = position.astype(f32) * inverse_ref[...]
        cos_ref[at, :] = jnp.cos(phase)
        sine = jnp.sin(phase)
        sin_ref[at, :] = jnp.where(lane % ROPE < ROPE // 2, -sine, sine)

    @pl.loop(0, slabs)
    def _(j):
        for k in range(2):
            b = exclusive(slab, j, slabs) * INNER + (twin + 2 * k) % INNER
            for copy in kv_copies(2, b, twin, False):
                copy.wait_recv()

    own[4].wait()
    own[5].wait()

    def project(k, latent, rope, first, size):
        lane = lax.broadcasted_iota(jnp.int32, (size, 128), 1)
        at = pl.ds(first, size)
        rope_even = jnp.where(lane < ROPE, rope, 0.0).astype(bf16)
        for h in range(0, heads, 2):
            pair = jnp.dot(latent, weights[0, k, :, h * NOPE : (h + 2) * NOPE], preferred_element_type=f32)
            keys[h, at, 0:128] = pair[:, :128].astype(bf16)
            keys[h, at, 128:256] = rope_even
            turned = pltpu.roll(pair[:, 128:], 64, 1)
            keys[h + 1, at, 0:128] = jnp.where(lane < ROPE, 0.0, turned).astype(bf16)
            keys[h + 1, at, 128:256] = jnp.where(lane < ROPE, turned, rope).astype(bf16)
            vals[at, h * VH : (h + 2) * VH] = jnp.dot(
                latent, weights[1, k, :, h * VH : (h + 2) * VH], preferred_element_type=f32
            ).astype(bf16)

    scale = math.log2(math.e) / math.sqrt(WIDTH)
    per_slab = chunks // half_slabs

    @pl.loop(0, 2)
    def _(k):
        @pl.when(k == 1)
        def _():
            @pl.loop(0, chunks)
            def _(i):
                w_beside(1 - piece, i).wait_recv()

        @pl.loop(0, C // csize)
        def _(i):
            first = pl.multiple_of(i * csize, csize)
            raw = kvc[pl.ds(first, csize), :]
            rope = raw[:, LATENT:].astype(f32)
            project(k, raw[:, :LATENT], jnp.concatenate([rope, rope], 1), first, csize)

        @pl.loop(0, T // tsize)
        def _(i):
            first = pl.multiple_of(i * tsize, tsize)
            at = pl.ds(first, tsize)
            raw = kvn[at, :]
            wide = raw[:, :LATENT].astype(f32)
            inv = lax.rsqrt(jnp.mean(wide * wide, axis=1, keepdims=True) + epsilon)
            latent = (wide * inv * gain_ref[...]).astype(bf16)
            rope = raw[:, LATENT:].astype(f32)
            rope = jnp.concatenate([rope, rope], 1)
            lane = lax.broadcasted_iota(jnp.int32, (tsize, 128), 1)
            rope = rope * cos_ref[at, :] + swap_halves(rope, lane) * sin_ref[at, :]
            project(k, latent, rope, pl.multiple_of(C + first, tsize), tsize)

        @pl.loop(0, half_slabs)
        def _(j):
            group = exclusive(slab, j + k * (half_slabs - 1 - 2 * j), slabs)

            @pl.loop(0, INNER)
            def _(i):
                b = group * INNER + i

                @pl.when(b != me)
                def _():
                    q_copy(k, me, b).wait_recv()

            base = pl.multiple_of(group * rows, rows)
            at = pl.ds(base, rows)
            near_at = pl.ds(pl.multiple_of(base - half_first * tok, rows), rows)
            row = base + lax.broadcasted_iota(jnp.int32, (rows, S), 0)
            col = lax.broadcasted_iota(jnp.int32, (rows, S), 1)
            live = ((col < C) & (col < plen_ref[0])) | ((col >= C) & (col - C <= row))
            bias[...] = jnp.where(live, 0.0, -1e30)

            @pl.loop(0, heads // 2)
            def _(p):
                lane = lax.broadcasted_iota(jnp.int32, (rows, 128), 1)
                cosine = cos_ref[at, :]
                sine = sin_ref[at, :]

                def third(i):
                    return qbuf[k, near_at, pl.ds(pl.multiple_of(p * 384 + 128 * i, 128), 128)]

                def turn(x, hit):
                    x = x.astype(f32)
                    y = x * cosine + swap_halves(x, lane) * sine
                    return jnp.where(hit, y, x).astype(bf16)

                front = third(0)
                middle = turn(third(1), lane < ROPE)
                back = turn(third(2), lane >= ROPE)
                for side, query in enumerate(
                    (jnp.concatenate([front, middle], 1), jnp.concatenate([middle, back], 1))
                ):
                    h = 2 * p + side
                    scores = lax.dot_general(
                        query, keys[h], (((1,), (1,)), ((), ())), preferred_element_type=f32
                    )
                    scores = scores * scale + bias[...]
                    top = jnp.max(scores, axis=1, keepdims=True)
                    grown = jnp.exp2(scores - top)
                    total = jnp.sum(grown, axis=1, keepdims=True)
                    across_v = pl.ds(pl.multiple_of(h * VH, VH), VH)
                    mixed = jnp.dot(grown.astype(bf16), vals[:, across_v], preferred_element_type=f32)
                    obuf[k, near_at, across_v] = (mixed / total).astype(bf16)

            @pl.loop(0, INNER)
            def _(i):
                b = group * INNER + i

                @pl.when(b != me)
                def _():
                    o_copy(k, b, me).start()

                @pl.when(b == me)
                def _():
                    own_out(k).start()

            @pl.when(k == 0)
            def _():
                @pl.loop(j * per_slab, (j + 1) * per_slab)
                def _(i):
                    w_direct(i).wait_recv()
                    w_beside(piece, i).start()

    for k in range(2):
        own_out(k).wait()

        @pl.loop(1, half)
        def _(i):
            peer = half_first + (me + i) % half
            q_copy(k, peer, me).wait_send()
            o_copy(k, peer, me).wait_send()
            o_copy(k, me, peer).wait_recv()

    @pl.loop(0, chunks)
    def _(i):
        w_direct(i).wait_send()
        w_beside(piece, i).wait_send()

    @pl.loop(0, slabs)
    def _(j):
        b = exclusive(slab, j, slabs) * INNER + inner

        @pl.when(j > 0)
        def _():
            for copy in kv_copies(0, me, b, True):
                copy.wait_send()

        for copy in kv_copies(1, b, across, False):
            copy.wait_send()
        for k in range(2):
            d = exclusive(slab, j, slabs) * INNER + (inner + 2 * k) % INNER
            for copy in kv_copies(2, d, twin, False):
                copy.wait_send()


PLANES = 4
EXTRA_END = 3
EXTRA_MIDDLE = 0
EXTRA_FAR = 1


def planes_kernel(
    n, tok, cac, heads,
    q_hbm, kvn_hbm, kvc_hbm, wk_hbm, wv_hbm, gain_ref, inverse_ref, plen_ref,
    out_hbm,
    qbuf, kvn, kvc, weights, latents, aux, keys, vals, bias, score_a, score_b, prob_a, prob_b, obuf,
    cos_ref, sin_ref,
    local_sem, own_w_sem, own_q_sem, own_out_sem, q_send, q_recv, kv_send, kv_recv, o_send, o_recv, w_send, w_recv,
):
    me = lax.axis_index("seq")
    part = lax.axis_index("groups")
    piece = part % 2
    plane = me // INNER
    inner = me % INNER
    side = plane // (PLANES // 2)
    last = PLANES - 1

    def whole(r):
        return r + side * (last - 2 * r)

    middle = whole(plane)
    end = middle == 0
    mid = middle == 1
    T, C = n * tok, n * cac
    S = T + C
    qw = heads * WIDTH
    ow = heads * VH
    rows = INNER * tok
    pairs = heads // 2
    f32, bf16 = jnp.float32, jnp.bfloat16
    scale = math.log2(math.e) / math.sqrt(WIDTH)

    def blk(ref, b, size):
        return ref.at[pl.ds(pl.multiple_of(b * size, size), size), :]

    def cols(ref, b, size):
        return ref.at[:, pl.ds(pl.multiple_of(b * size, 128), size)]

    def head_plane(k):
        return whole(jnp.where(end, k, jnp.where(k == 0, 1, jnp.where(k == 1, 0, k))))

    steps = 3 + middle

    def own_q(k):
        return pltpu.make_async_copy(
            cols(q_hbm, head_plane(k) * INNER + inner, qw), blk(qbuf.at[k], inner, tok), own_q_sem.at[k]
        )

    own = [
        pltpu.make_async_copy(kvn_hbm, blk(kvn, me, tok), local_sem.at[0]),
        pltpu.make_async_copy(kvc_hbm, blk(kvc, me, cac), local_sem.at[1]),
    ]
    for copy in own:
        copy.start()

    def own_w(which, i):
        source = wv_hbm if which else wk_hbm
        return pltpu.make_async_copy(cols(source, i, 2 * NOPE), weights.at[0, which, i], own_w_sem.at[which, i])

    for which in range(2):
        @pl.loop(0, pairs)
        def _(i):
            own_w(which, i).start()

    barrier = pltpu.get_barrier_semaphore()

    @pl.loop(1, n)
    def _(i):
        pl.semaphore_signal(barrier, inc=1, device_id={"seq": (me + i) % n})

    beside = {"groups": part + 1 - 2 * piece, "seq": me}
    pl.semaphore_signal(barrier, inc=1, device_id=beside)
    pl.semaphore_wait(barrier, n)

    def kv_copies(stage, b, peer, from_hbm):
        slot = b if stage else peer
        return [
            pltpu.make_async_remote_copy(
                src_ref=kvn_hbm if from_hbm else blk(kvn, b, tok),
                dst_ref=blk(kvn, b, tok),
                send_sem=kv_send.at[2 * stage, slot],
                recv_sem=kv_recv.at[0, b],
                device_id={"seq": peer},
            ),
            pltpu.make_async_remote_copy(
                src_ref=kvc_hbm if from_hbm else blk(kvc, b, cac),
                dst_ref=blk(kvc, b, cac),
                send_sem=kv_send.at[2 * stage + 1, slot],
                recv_sem=kv_recv.at[1, b],
                device_id={"seq": peer},
            ),
        ]

    near = {"seq": whole(1 - middle) * INNER + inner}
    beyond = {"seq": whole(2) * INNER + inner}

    def far_query(source):
        return pltpu.make_async_remote_copy(
            src_ref=blk(qbuf.at[PLANES], source, tok),
            dst_ref=blk(qbuf.at[PLANES], source, tok),
            send_sem=q_send.at[PLANES + 1, source],
            recv_sem=q_recv.at[PLANES, source],
            device_id=near,
        )

    def q_copy(k, to_plane, to, source):
        columns = jnp.where(k == PLANES, whole(last), head_plane(k)) * INNER + to
        return pltpu.make_async_remote_copy(
            src_ref=cols(q_hbm, columns, qw),
            dst_ref=blk(qbuf.at[k], source, tok),
            send_sem=q_send.at[k, to],
            recv_sem=q_recv.at[k, source],
            device_id={"seq": to_plane * INNER + to},
        )

    def o_part(k, part_of, to):
        return obuf.at[k, pl.ds(pl.multiple_of(to * tok, tok), tok), pl.ds(pl.multiple_of(part_of * ow // 2, 128), ow // 2)]

    def o_copy(k, part_of, to_plane, to, source):
        columns = jnp.where(k == PLANES, whole(last), head_plane(k)) * INNER + source
        return pltpu.make_async_remote_copy(
            src_ref=o_part(k, part_of, to),
            dst_ref=cols(out_hbm, 2 * columns + part_of, ow // 2),
            send_sem=o_send.at[k, part_of, to],
            recv_sem=o_recv.at[k, part_of, source],
            device_id={"seq": to_plane * INNER + to},
        )

    def own_out(k, part_of):
        columns = head_plane(k) * INNER + inner
        return pltpu.make_async_copy(
            o_part(k, part_of, inner), cols(out_hbm, 2 * columns + part_of, ow // 2), own_out_sem.at[k, part_of]
        )

    def w_chunk(k, which, i):
        return weights.at[k, which, i]

    def w_copy(way, k, to_k, which, i, device):
        return pltpu.make_async_remote_copy(
            src_ref=w_chunk(k, which, i),
            dst_ref=w_chunk(to_k, which, i),
            send_sem=w_send.at[way, k, which, i],
            recv_sem=w_recv.at[to_k, which, i],
            device_id=device,
        )

    def w_near(k, which, i):
        return w_copy(0, k, jnp.where(k == 0, 1, 2), which, i, near)

    def w_beyond(k, which, i):
        return w_copy(1, k, k + 2, which, i, beyond)

    def w_beside(k, i):
        return w_copy(2, k, k, piece, i, beside)

    def extras(k):
        return jnp.where(mid, jnp.where(k == 1, EXTRA_END, jnp.where(k == 2, EXTRA_MIDDLE, EXTRA_FAR)), 0)

    late_pair = pairs - 2

    def for_own_weights(do):
        @pl.loop(0, pairs)
        def _(i):
            do(w_near(0, piece, i))

            @pl.when(mid)
            def _():
                do(w_beyond(0, piece, i))

        @pl.when(end)
        def _():
            @pl.loop(pairs - EXTRA_END, pairs)
            def _(i):
                @pl.when(i != late_pair)
                def _():
                    do(w_near(0, 1 - piece, i))

        @pl.when(mid)
        def _():
            @pl.loop(pairs - EXTRA_MIDDLE, pairs)
            def _(i):
                do(w_beyond(0, 1 - piece, i))

    def for_forwards(k, i, do):
        @pl.when(mid & (k == 1))
        def _():
            do(w_beyond(k, piece, i))

        @pl.when(mid & (k == 2))
        def _():
            do(w_near(k, piece, i))

        @pl.when(i < pairs - extras(k))
        def _():
            do(w_beside(k, i))

    def pass_on(k, i):
        w_copy(2, k, k, piece, i, beside).wait_recv()
        for_forwards(k, i, lambda copy: copy.start())

    @pl.loop(1, PLANES)
    def _(j):
        for copy in kv_copies(0, me, exclusive(plane, j, PLANES) * INNER + inner, True):
            copy.start()

    for which in range(2):
        @pl.loop(0, pairs)
        def _(i):
            own_w(which, i).wait()

    for_own_weights(lambda copy: copy.start())

    across = plane * INNER + (inner + 2) % INNER
    twin = me + 1 - 2 * (me % 2)
    own[0].wait()
    own[1].wait()

    own_far_q = pltpu.make_async_copy(
        cols(q_hbm, whole(last) * INNER + inner, qw), blk(qbuf.at[PLANES], inner, tok), local_sem.at[2]
    )

    @pl.when(end)
    def _():
        own_far_q.start()

    @pl.loop(0, steps)
    def _(k):
        own_q(k).start()

    def for_queries(k, do):
        @pl.loop(1, INNER)
        def _(i):
            do(q_copy(k, plane, (inner + i) % INNER, inner))

    def relay_kv(p):
        b = p * INNER + inner
        for copy in kv_copies(1, b, across, False):
            copy.start()
        for copy in kv_copies(2, b, twin, False):
            copy.start()

    relay_kv(plane)
    @pl.loop(1, PLANES)
    def _(j):
        p = exclusive(plane, j, PLANES)
        for copy in kv_copies(0, p * INNER + inner, twin, False):
            copy.wait_recv()
        relay_kv(p)

    for_queries(0, lambda copy: copy.start())

    @pl.when(end)
    def _():
        for_queries(PLANES, lambda copy: copy.start())
        for_queries(1, lambda copy: copy.start())
        for_queries(2, lambda copy: copy.start())

    @pl.when(mid)
    def _():
        for k in (2, 1, 3):
            for_queries(k, lambda copy: copy.start())

    tsize = math.gcd(T, 256)
    csize = math.gcd(C, 256)

    @pl.loop(0, T // tsize)
    def _(i):
        first = pl.multiple_of(i * tsize, tsize)
        at = pl.ds(first, tsize)
        lane = lax.broadcasted_iota(jnp.int32, (tsize, 128), 1)
        position = plen_ref[0] + first + lax.broadcasted_iota(jnp.int32, (tsize, 128), 0)
        phase = position.astype(f32) * inverse_ref[...]
        cos_ref[at, :] = jnp.cos(phase)
        sine = jnp.sin(phase)
        sin_ref[at, :] = jnp.where(lane % ROPE < ROPE // 2, -sine, sine)

    bias[...] = jnp.where(
        lax.broadcasted_iota(jnp.int32, (rows, rows), 1) <= lax.broadcasted_iota(jnp.int32, (rows, rows), 0),
        0.0, -1e30,
    )

    def pass_on_near(i):
        pass_on(1, i)

        @pl.when(mid)
        def _():
            pass_on(2, i)

    pass_on_near(0)

    @pl.loop(0, PLANES)
    def _(j):
        b = exclusive(plane, j, PLANES) * INNER + (inner + 2) % INNER
        for copy in kv_copies(1, b, twin, False):
            copy.wait_recv()
        for copy in kv_copies(2, b, twin, False):
            copy.start()

    pass_on_near(1)

    @pl.loop(0, heads)
    def _(h):
        vals[h, :, 128:256] = jnp.ones((S, 128), bf16)

    @pl.loop(0, PLANES)
    def _(j):
        for k in range(2):
            b = exclusive(plane, j, PLANES) * INNER + (twin + 2 * k) % INNER
            for copy in kv_copies(2, b, twin, False):
                copy.wait_recv()

    def keep_rope(first, size, rope, dead):
        at = pl.ds(first, size)
        lane = lax.broadcasted_iota(jnp.int32, (size, 128), 1)
        low = lane < ROPE
        aux[at, :] = jnp.where(low, jnp.where(lane == 0, dead, 0.0), rope)
        tail = jnp.where(low, rope, jnp.where(lane == ROPE, dead, 0.0)).astype(bf16)
        for h in range(0, heads, 2):
            keys[h, at, 128:256] = tail

    @pl.loop(0, C // csize)
    def _(i):
        first = pl.multiple_of(i * csize, csize)
        raw = kvc[pl.ds(first, csize), :]
        latents[pl.ds(first, csize), :] = raw[:, :LATENT]
        rope = raw[:, LATENT:].astype(f32)
        row = first + lax.broadcasted_iota(jnp.int32, (csize, 128), 0)
        dead = jnp.where(row < plen_ref[0], 0.0, -1e30)
        keep_rope(first, csize, jnp.concatenate([rope, rope], 1), dead)

    @pl.loop(0, T // tsize)
    def _(i):
        first = pl.multiple_of(i * tsize, tsize)
        at = pl.ds(first, tsize)
        raw = kvn[at, :]
        wide = raw[:, :LATENT].astype(f32)
        inv = lax.rsqrt(jnp.mean(wide * wide, axis=1, keepdims=True) + epsilon)
        latents[pl.ds(pl.multiple_of(C + first, tsize), tsize), :] = (wide * inv * gain_ref[...]).astype(bf16)
        rope = raw[:, LATENT:].astype(f32)
        rope = jnp.concatenate([rope, rope], 1)
        lane = lax.broadcasted_iota(jnp.int32, (tsize, 128), 1)
        rope = rope * cos_ref[at, :] + swap_halves(rope, lane) * sin_ref[at, :]
        keep_rope(pl.multiple_of(C + first, tsize), tsize, rope, 0.0)
        cos_ref[at, :] = cos_ref[at, :] * scale
        sin_ref[at, :] = sin_ref[at, :] * scale

    pass_on_near(2)
    size = math.gcd(C, rows)

    def project_rows(k, p, live):
        lane = lax.broadcasted_iota(jnp.int32, (size, 128), 1)
        for first in range(0, live, size):
            at = slice(first, first + size)
            latent = latents[at, :]
            rest = aux[at, :]
            pair = jnp.dot(latent, weights[k, 0, p], preferred_element_type=f32) * scale
            keys[2 * p, at, 0:128] = pair[:, :128].astype(bf16)
            turned = pltpu.roll(pair[:, 128:], 64, 1)
            keys[2 * p + 1, at, 0:128] = jnp.where(lane < ROPE, rest, turned).astype(bf16)
            keys[2 * p + 1, at, 128:256] = jnp.where(lane < ROPE, turned, rest).astype(bf16)
            both = jnp.dot(latent, weights[k, 1, p], preferred_element_type=f32).astype(bf16)
            vals[2 * p, at, 0:128] = both[:, :128]
            vals[2 * p + 1, at, 0:128] = both[:, 128:]

    def project(k, p):
        top_plane = jnp.where(mid & (k == last), jnp.maximum(plane, whole(0)), plane)
        for s in range(PLANES):
            @pl.when(top_plane == s)
            def _():
                project_rows(k, p, C + (s + 1) * rows)

    def attend(slot, first_row, live, first_pair, last_pair):
        cut = live - rows

        def rotated(p):
            at = pl.ds(first_row, rows)
            lane = lax.broadcasted_iota(jnp.int32, (rows, 128), 1)
            cosine = cos_ref[at, :]
            sine = sin_ref[at, :]

            def third(i):
                return qbuf[slot, :, pl.ds(pl.multiple_of(p * 3 * 128 + 128 * i, 128), 128)]

            def turn(x, hit):
                x = x.astype(f32)
                y = x * cosine + swap_halves(x, lane) * sine
                return jnp.where(hit, y, x)

            centre = turn(third(1), lane < ROPE)
            return (
                jnp.concatenate([third(0), jnp.where(lane == ROPE, 1.0, centre).astype(bf16)], 1),
                jnp.concatenate(
                    [jnp.where(lane == 0, 1.0, centre).astype(bf16), turn(third(2), lane >= ROPE).astype(bf16)], 1
                ),
            )

        def score(query, h, into):
            into[:, 0:live] = lax.dot_general(
                query, keys[h, 0:live, :], (((1,), (1,)), ((), ())), preferred_element_type=f32
            )

        def soften(scores, into):
            for r in range(0, rows, 16):
                before = scores[r : r + 16, 0:cut]
                near_end = scores[r : r + 16, cut:live] + bias[r : r + 16, :]
                top = jnp.maximum(
                    jnp.max(before, axis=1, keepdims=True), jnp.max(near_end, axis=1, keepdims=True)
                )
                into[r : r + 16, 0:cut] = jnp.exp2(before - top).astype(bf16)
                into[r : r + 16, cut:live] = jnp.exp2(near_end - top).astype(bf16)

        def mix(probs, h):
            mixed = jnp.dot(probs[:, 0:live], vals[h, 0:live, :], preferred_element_type=f32)
            obuf[slot, :, pl.ds(pl.multiple_of(h * VH, VH), VH)] = (mixed[:, :VH] / mixed[:, VH:]).astype(bf16)

        @pl.loop(first_pair, last_pair)
        def _(p):
            done = jnp.maximum(p - 1, first_pair)
            even, odd = rotated(p)
            score(even, 2 * p, score_a)
            soften(score_b, prob_b)
            mix(prob_a, 2 * done)
            soften(score_a, prob_a)
            mix(prob_b, 2 * done + 1)
            score(odd, 2 * p + 1, score_b)

        soften(score_b, prob_b)
        mix(prob_a, 2 * last_pair - 2)
        mix(prob_b, 2 * last_pair - 1)

    def attend_plane(slot, s, first_pair, last_pair):
        for plane_of in range(PLANES):
            @pl.when(s == plane_of)
            def _():
                attend(slot, plane_of * rows, C + (plane_of + 1) * rows, first_pair, last_pair)

    def other_kind(k, p):
        return w_copy(2, k, k, 1 - piece, p, beside)

    @pl.loop(0, jnp.where(end, 5, 7))
    def _(turn):
        ends_k = 1 + (turn - 1) // 2
        mids_k = jnp.where(turn <= 2, 2, jnp.where((turn == 3) | (turn == 6), 1, last))
        k = jnp.where(turn == 0, 0, jnp.where(end, ends_k, mids_k))
        ends_half = (turn + 1) % 2
        mids_half = jnp.where((turn == 2) | (turn >= 5), 1, 0)
        half = jnp.where(turn == 0, 0, jnp.where(end, ends_half, mids_half))
        far = mid & (k == last)
        first_pair = half * (pairs // 2)
        last_pair = jnp.where(turn == 0, pairs, first_pair + pairs // 2)

        @pl.when(mid & (turn == 5))
        def _():
            pass_on(3, 3)

        @pl.loop(first_pair, last_pair)
        def _(p):
            @pl.when((k > 0) & ~(mid & (k == 1) & (p >= pairs - EXTRA_FAR)))
            def _():
                other_kind(k, p).wait_recv()

            project(k, p)

        @pl.when(half == 0)
        def _():
            own_q(k).wait()

            @pl.loop(1, INNER)
            def _(i):
                q_copy(k, plane, inner, (inner + i) % INNER).wait_recv()

        @pl.when(turn == 0)
        def _():
            pass_on_near(3)

        @pl.when(end & (turn == 3))
        def _():
            pass_on(2, 2)

        @pl.loop(jnp.where(far, 0, 1), 2)
        def _(item):
            far_item = far & (item == jnp.where(turn == 5, 0, 1))

            @pl.when(far_item & (turn == 4))
            def _():
                @pl.loop(0, INNER)
                def _(i):
                    far_query(i).wait_recv()

            slot = jnp.where(far_item, PLANES, k)
            attend_plane(slot, jnp.where(far_item, whole(0), plane), first_pair, last_pair)

            @pl.loop(first_pair // (pairs // 2), last_pair // (pairs // 2))
            def _(part_of):
                @pl.when(far_item)
                def _():
                    @pl.loop(0, INNER)
                    def _(i):
                        o_copy(PLANES, part_of, whole(0), (inner + i) % INNER, inner).start()

                @pl.when(~far_item)
                def _():
                    own_out(k, part_of).start()

                    @pl.loop(1, INNER)
                    def _(i):
                        o_copy(k, part_of, plane, (inner + i) % INNER, inner).start()

        @pl.when(end & (turn > 0) & (turn < 4))
        def _():
            pass_on(2, jnp.where(turn == 3, 3, turn - 1))

        @pl.when(mid & ((turn < 2) | (turn == 3)))
        def _():
            pass_on(3, jnp.where(turn == 3, 2, turn))

        @pl.when(mid & (turn == 1))
        def _():
            @pl.loop(pairs - EXTRA_FAR, pairs)
            def _(p):
                other_kind(1, p).wait_recv()
                w_beyond(1, 1 - piece, p).start()

        @pl.when(end & (turn == 0))
        def _():
            @pl.loop(1, INNER)
            def _(i):
                q_copy(PLANES, plane, inner, (inner + i) % INNER).wait_recv()

            own_far_q.wait()

            @pl.loop(0, INNER)
            def _(i):
                far_query(i).start()

            w_near(0, 1 - piece, late_pair).start()

    @pl.loop(0, 2)
    def _(part_of):
        @pl.loop(0, steps)
        def _(k):
            own_out(k, part_of).wait()

            @pl.loop(1, INNER)
            def _(i):
                o_copy(k, part_of, plane, (inner + i) % INNER, inner).wait_send()
                o_copy(k, part_of, plane, inner, (inner + i) % INNER).wait_recv()

        @pl.when(mid)
        def _():
            @pl.loop(0, INNER)
            def _(i):
                o_copy(PLANES, part_of, whole(0), (inner + i) % INNER, inner).wait_send()

        @pl.when(end)
        def _():
            @pl.loop(0, INNER)
            def _(i):
                o_copy(PLANES, part_of, plane, inner, i).wait_recv()

    @pl.loop(0, steps)
    def _(k):
        for_queries(k, lambda copy: copy.wait_send())

    @pl.when(end)
    def _():
        for_queries(PLANES, lambda copy: copy.wait_send())

        @pl.loop(0, INNER)
        def _(i):
            far_query(i).wait_send()

        w_near(0, 1 - piece, late_pair).wait_send()

    for_own_weights(lambda copy: copy.wait_send())

    @pl.when(mid)
    def _():
        @pl.loop(pairs - EXTRA_FAR, pairs)
        def _(i):
            w_beyond(1, 1 - piece, i).wait_send()

    @pl.loop(1, steps)
    def _(k):
        @pl.loop(0, pairs)
        def _(i):
            for_forwards(k, i, lambda copy: copy.wait_send())

    @pl.loop(0, PLANES)
    def _(j):
        b = exclusive(plane, j, PLANES) * INNER + inner

        @pl.when(j > 0)
        def _():
            for copy in kv_copies(0, me, b, True):
                copy.wait_send()

        for copy in kv_copies(1, b, across, False):
            copy.wait_send()
        for k in range(2):
            d = exclusive(plane, j, PLANES) * INNER + (inner + 2 * k) % INNER
            for copy in kv_copies(2, d, twin, False):
                copy.wait_send()


def local_any(n, queries, kv_new, kv_cache, kv_gain, w_key, w_value, prefix_len):
    tok = queries.shape[0]
    cac = kv_cache.shape[0]
    heads = w_key.shape[1] // NOPE
    T, C = n * tok, n * cac
    chunks = max(4, n // (2 * INNER))
    hbm = pl.BlockSpec(memory_space=pl.ANY)
    vmem = pl.BlockSpec(memory_space=pltpu.VMEM)
    bf16 = jnp.bfloat16
    dma = pltpu.SemaphoreType.DMA
    return pl.pallas_call(
        functools.partial(kernel, n, tok, cac, heads, chunks),
        out_shape=jax.ShapeDtypeStruct((tok, n * heads * VH), bf16),
        in_specs=[hbm] * 5 + [vmem] * 2 + [pl.BlockSpec(memory_space=pltpu.SMEM)],
        out_specs=hbm,
        scratch_shapes=[
            pltpu.VMEM((2, T // 2, heads * WIDTH), bf16),
            pltpu.VMEM((T, LATENT + ROPE), bf16),
            pltpu.VMEM((C, LATENT + ROPE), bf16),
            pltpu.VMEM((2, 2, LATENT, heads * NOPE), bf16),
            pltpu.VMEM((heads, C + T, 256), bf16),
            pltpu.VMEM((C + T, heads * VH), bf16),
            pltpu.VMEM((INNER * tok, C + T), jnp.float32),
            pltpu.VMEM((2, T // 2, heads * VH), bf16),
            pltpu.VMEM((T, 128), jnp.float32),
            pltpu.VMEM((T, 128), jnp.float32),
            dma((6,)),
            dma((2,)),
            dma((2, n)),
            dma((2, n)),
            dma((6, n)),
            dma((2, n)),
            dma((2, n)),
            dma((2, n)),
            dma((2, chunks)),
            dma((2, chunks)),
        ],
        compiler_params=pltpu.CompilerParams(
            collective_id=0, has_side_effects=True, vmem_limit_bytes=60 * 2**20
        ),
        name="latent_attention",
    )(queries, kv_new, kv_cache, w_key, w_value, kv_gain[None, :], inverse_lanes(), prefix_len)


def local_planes(n, queries, kv_new, kv_cache, kv_gain, w_key, w_value, prefix_len):
    tok = queries.shape[0]
    cac = kv_cache.shape[0]
    heads = w_key.shape[1] // NOPE
    T, C = n * tok, n * cac
    S = T + C
    rows = INNER * tok
    pairs = heads // 2
    hbm = pl.BlockSpec(memory_space=pl.ANY)
    vmem = pl.BlockSpec(memory_space=pltpu.VMEM)
    bf16, f32 = jnp.bfloat16, jnp.float32
    dma = pltpu.SemaphoreType.DMA
    return pl.pallas_call(
        functools.partial(planes_kernel, n, tok, cac, heads),
        out_shape=jax.ShapeDtypeStruct((tok, n * heads * VH), bf16),
        in_specs=[hbm] * 5 + [vmem] * 2 + [pl.BlockSpec(memory_space=pltpu.SMEM)],
        out_specs=hbm,
        scratch_shapes=[
            pltpu.VMEM((PLANES + 1, rows, heads * WIDTH), bf16),
            pltpu.VMEM((T, LATENT + ROPE), bf16),
            pltpu.VMEM((C, LATENT + ROPE), bf16),
            pltpu.VMEM((PLANES, 2, pairs, LATENT, 2 * NOPE), bf16),
            pltpu.VMEM((S, LATENT), bf16),
            pltpu.VMEM((S, 128), f32),
            pltpu.VMEM((heads, S, 256), bf16),
            pltpu.VMEM((heads, S, 256), bf16),
            pltpu.VMEM((rows, rows), f32),
            pltpu.VMEM((rows, S), f32),
            pltpu.VMEM((rows, S), f32),
            pltpu.VMEM((rows, S), bf16),
            pltpu.VMEM((rows, S), bf16),
            pltpu.VMEM((PLANES + 1, rows, heads * VH), bf16),
            pltpu.VMEM((T, 128), f32),
            pltpu.VMEM((T, 128), f32),
            dma((3,)),
            dma((2, pairs)),
            dma((PLANES,)),
            dma((PLANES, 2)),
            dma((PLANES + 2, INNER)),
            dma((PLANES + 1, INNER)),
            dma((6, n)),
            dma((2, n)),
            dma((PLANES + 1, 2, INNER)),
            dma((PLANES + 1, 2, INNER)),
            dma((3, PLANES, 2, pairs)),
            dma((PLANES, 2, pairs)),
        ],
        compiler_params=pltpu.CompilerParams(
            collective_id=0, has_side_effects=True, vmem_limit_bytes=60 * 2**20
        ),
        name="latent_attention",
    )(queries, kv_new, kv_cache, w_key, w_value, kv_gain[None, :], inverse_lanes(), prefix_len)


def local(n, *operands):
    run = local_planes if n == PLANES * INNER else local_any
    return run(n, *operands)


def solution(mesh):
    placed = (
        P(("groups", "seq"), None),
        P(("groups", "seq"), None),
        P(("groups", "seq"), None),
        P(),
        P(None, "seq"),
        P(None, "seq"),
        P("groups"),
    )
    return jax.shard_map(
        functools.partial(local, mesh.shape["seq"]),
        mesh=mesh,
        in_specs=placed,
        out_specs=P(("groups", "seq"), None),
        check_vma=False,
    )
```
